32 devices in a mesh: dp: 8 (over y, x, core), mp: 4 (over z).
Axes of the slice: x: 2, y: 2, z: 4, core: 2. Of those that a mesh axis runs over, the one named last changes fastest.
Arguments:
- inputs: bfloat16 [1024, 6144], P('dp'), may hold values from -6 to 6
- pre_act: bfloat16 [1024, 12288], P('dp', 'mp'), may hold values from -6 to 6
- out_grad: bfloat16 [1024, 6144], P('dp'), may hold values from -6 to 6
- w_in: bfloat16 [6144, 12288], P(None, 'mp'), may hold values from -0.109375 to 0.109375
- w_out: bfloat16 [12288, 6144], P('mp'), may hold values from -0.0546875 to 0.0546875
- master_in: float32 [6144, 12288], P('dp', 'mp'), may hold values from -0.3 to 0.3
- master_out: float32 [12288, 6144], P('mp', 'dp'), may hold values from -0.3 to 0.3
- row_in: float32 [6144], P('dp'), may hold values from 12.8 to 686.08
- col_in: float32 [12288], P('mp'), may hold values from 25 to 128
- row_out: float32 [12288], P('mp'), may hold values from 25.6 to 1372.16
- col_out: float32 [6144], P('dp'), may hold values from 51 to 256
Outputs:
- input_grad: bfloat16 [1024, 6144], P('dp', 'mp')
- new_master_in: float32 [6144, 12288], P('dp', 'mp')
- new_master_out: float32 [12288, 6144], P('mp', 'dp')
The draws below stay inside these ranges and needn't reach their ends.
All inputs are finite; a program needn't handle non-finite values.
Results may differ from the reference program's by a relative error of at most 0.012.
Values may be sent and summed in bfloat16 or wider, within the bound.
A program may use at most 256 MiB of HBM per device.

```python
import math
import jax
import jax.numpy as jnp
from jax import lax

D = 6144
FF = 12288
TOK_DEV = 128
TOKENS = 1024
N_DP = 8


def falling_factor(key, count, high, ratio):
    place = jnp.arange(count, dtype=jnp.float32) / float(count)
    noise = jax.random.uniform(key, (count,), jnp.float32, -0.28, 0.28)
    return high * jnp.exp(-jnp.log(ratio) * place + noise)


def draw_row_in(key, part):
    return falling_factor(jax.random.fold_in(key, 11), D, TOKENS * 0.5, 10.0)


def draw_row_out(key, part):
    return falling_factor(jax.random.fold_in(key, 23), FF, TOKENS * 1.0, 10.0)


def spiked(entries, key, source, target, blocks, factor):
    owner, partner = [(jnp.arange(entries.shape[position]) // (entries.shape[position] // blocks)).reshape([-1 if axis == position else 1 for axis in range(entries.ndim)]) for position in (source, target)]
    chosen = jax.random.permutation(key, blocks)[partner]
    strong = (owner == chosen) | (owner == (partner + blocks // 2) % blocks)
    return jnp.where(strong, factor * entries, entries)


def levels(rng, extent, cuts, least, high):
    loudness, own = 1.0, jax.random.fold_in(rng, 6)
    for position, blocks in cuts:
        heights = jnp.exp(jax.random.uniform(jax.random.fold_in(own, position), (blocks,), jnp.float32, least / len(cuts), high / len(cuts)))
        loudness = loudness * jnp.repeat(heights, extent[position] // blocks).reshape([-1 if axis == position else 1 for axis in range(len(extent))])
    return loudness


def scatter_about(stream_key, extent, width, most, shards=(), held_as=jnp.bfloat16):
    entries = width * jax.random.normal(stream_key, extent, jnp.float32)
    if shards:
        entries = entries * levels(stream_key, extent, shards, -0.22, 0.18)
    return jnp.clip(entries, -most, most).astype(held_as)


def noise_with(rng, dims, deviation, reach, cuts, heavy, held_as=jnp.bfloat16):
    drawn = deviation * jax.random.normal(rng, dims, jnp.float32)
    if cuts:
        drawn = drawn * levels(rng, dims, cuts, -0.22, 0.18)
    return jnp.clip(spiked(drawn, jax.random.fold_in(rng, 3), *heavy), -reach, reach).astype(held_as)


def setup_inputs(seed: int = 0) -> dict:
    keys = jax.random.split(jax.random.key(seed), 12)
    inputs = noise_with(keys[0], (TOKENS, D), 1.0, 6.0, ((0, 8),), (0, 1, 8, 2.0))
    pre_act = scatter_about(keys[1], (TOKENS, FF), 1.0, 6.0, ((0, 8), (1, 4)))
    out_grad = noise_with(keys[2], (TOKENS, D), 1.0, 6.0, ((0, 8),), (0, 1, 8, 2.0))
    w_in = noise_with(keys[3], (D, FF), D ** -0.5, 0.109375, ((1, 4),), (1, 0, 4, 2.0))
    w_out = scatter_about(keys[4], (FF, D), FF ** -0.5, 0.0546875, ((0, 4),))
    master_in = scatter_about(keys[5], (D, FF), 0.05, 0.3, ((0, 8), (1, 4)), jnp.float32)
    master_out = scatter_about(keys[6], (FF, D), 0.05, 0.3, ((0, 4), (1, 8)), jnp.float32)
    row_in = draw_row_in(jax.random.fold_in(keys[11], 71), 0)
    col_in = jnp.clip(jnp.exp(math.log(128.0) - 1.6331544 * jax.random.uniform(keys[8], (FF,), jnp.float32) ** levels(keys[8], (FF,), ((0, 4),), -0.2, 0.2)), 25.0, 128.0)
    row_out = draw_row_out(jax.random.fold_in(keys[11], 71), 0)
    col_out = jnp.clip(jnp.exp(math.log(256.0) - 1.6133518 * jax.random.uniform(keys[10], (D,), jnp.float32) ** levels(keys[10], (D,), ((0, 8),), -0.2, 0.2)), 51.0, 256.0)
    return dict(inputs=inputs, pre_act=pre_act, out_grad=out_grad, w_in=w_in, w_out=w_out, master_in=master_in, master_out=master_out, row_in=row_in, col_in=col_in, row_out=row_out, col_out=col_out)


decay_rate = 0.8
step_size = 0.05
tiny_square = 1e-30

def gelu_parts(pre):
    cumulative = 0.5 * (1.0 + jax.scipy.special.erf(pre * (1.0 / math.sqrt(2.0))))
    density = jnp.exp(-0.5 * pre * pre) * (1.0 / math.sqrt(2.0 * math.pi))
    return (pre * cumulative, cumulative + pre * density)

def adafactor(grad, master, row_state, col_state):
    square = grad * grad + tiny_square
    row_new = decay_rate * row_state + (1.0 - decay_rate) * lax.optimization_barrier(jnp.mean(square, axis=1))
    col_new = decay_rate * col_state + (1.0 - decay_rate) * lax.optimization_barrier(jnp.mean(square, axis=0))
    second = row_new[:, None] * col_new[None, :] / jnp.mean(row_new)
    update = grad / jnp.sqrt(second)
    return master - step_size * update

def reference(inputs, pre_act, out_grad, w_in, w_out, master_in, master_out, row_in, col_in, row_out, col_out):
    active, slope = gelu_parts(pre_act.astype(jnp.float32))
    hidden = active.astype(jnp.bfloat16)
    hid_grad = jnp.dot(out_grad, w_out.T, preferred_element_type=jnp.float32)
    pre_grad = (hid_grad * slope).astype(jnp.bfloat16)
    input_grad = jnp.dot(pre_grad, w_in.T, preferred_element_type=jnp.float32).astype(jnp.bfloat16)

    def group(totals, index):
        begin = (index * TOK_DEV).astype(jnp.int32)
        rows_x = lax.dynamic_slice_in_dim(inputs, begin, TOK_DEV, 0)
        rows_g = lax.dynamic_slice_in_dim(pre_grad, begin, TOK_DEV, 0)
        rows_h = lax.dynamic_slice_in_dim(hidden, begin, TOK_DEV, 0)
        rows_y = lax.dynamic_slice_in_dim(out_grad, begin, TOK_DEV, 0)
        part_in = jnp.dot(rows_x.T, rows_g, preferred_element_type=jnp.float32).astype(jnp.bfloat16)
        part_out = jnp.dot(rows_h.T, rows_y, preferred_element_type=jnp.float32).astype(jnp.bfloat16)
        part_in, part_out = lax.optimization_barrier((part_in, part_out))
        return ((totals[0] + part_in.astype(jnp.float32), totals[1] + part_out.astype(jnp.float32)), None)
    start_sums = (jnp.zeros((D, FF), jnp.float32), jnp.zeros((FF, D), jnp.float32))
    (grad_in, grad_out), _ = lax.scan(group, start_sums, jnp.arange(N_DP, dtype=jnp.int32))
    new_master_in = adafactor(grad_in, master_in, row_in, col_in)
    new_master_out = adafactor(grad_out, master_out, row_out, col_out)
    return (input_grad, new_master_in, new_master_out)
```

```python
import functools
import math

import jax
import jax.numpy as jnp
from jax import lax
from jax.experimental import pallas as pl
from jax.experimental.pallas import tpu as pltpu
from jax.experimental.layout import Layout, with_layout_constraint
from jax.sharding import PartitionSpec as P

D = 6144
FF = 12288


decay_rate = 0.8
step_size = 0.05
tiny_square = 1e-30


def gelu_parts(pre):
    cumulative = 0.5 * (1.0 + jax.scipy.special.erf(pre * (1.0 / math.sqrt(2.0))))
    density = jnp.exp(-0.5 * pre * pre) * (1.0 / math.sqrt(2.0 * math.pi))
    return (pre * cumulative, cumulative + pre * density)


def contract_rows(left, right):
    return lax.dot_general(
        left, right, (((0,), (0,)), ((), ())), preferred_element_type=jnp.float32
    )


def scatter_pieces(partial, axis):
    size = lax.axis_size(axis)
    me = lax.axis_index(axis)
    width = partial.shape[1] // size
    piece = lambda k: lax.dynamic_slice_in_dim(partial, k * width, width, 1)
    pieces = [piece(me)]
    for shift in range(1, size):
        moved = piece(lax.rem(me + shift, size)).astype(jnp.bfloat16)
        pieces.append(lax.ppermute(moved, axis, [(i, (i + shift) % size) for i in range(size)]))
    return pieces


def body(
    inputs, pre_act, out_grad, w_in, w_out, master_in, master_out, row_in, col_in, row_out, col_out
):
    active, slope = gelu_parts(pre_act.astype(jnp.float32))
    hidden = active.astype(jnp.bfloat16)
    hidden_all = lax.all_gather(hidden, "dp", axis=0, tiled=True)
    out_grad, _ = lax.optimization_barrier((out_grad, hidden))
    out_cols = lax.all_to_all(out_grad, "dp", 1, 0, tiled=True)
    hid_grad = lax.dot_general(
        out_grad, w_out, (((1,), (1,)), ((), ())), preferred_element_type=jnp.float32
    )
    pre_grad = (hid_grad * slope).astype(jnp.bfloat16)
    pre_grad_all = lax.all_gather(pre_grad, "dp", axis=0, tiled=True)
    input_part = lax.dot_general(
        pre_grad, w_in, (((1,), (1,)), ((), ())), preferred_element_type=jnp.float32
    )
    inputs, input_part = lax.optimization_barrier((inputs, input_part))
    in_cols = lax.all_to_all(inputs, "dp", 1, 0, tiled=True)
    pieces = scatter_pieces(input_part, "mp")

    grad_out = contract_rows(hidden_all, out_cols)
    square_out = grad_out * grad_out + tiny_square
    width_out, row_out_sum = lax.psum((jnp.sum(square_out, axis=0), jnp.sum(row_out)), "mp")
    cols_out = decay_rate * col_out + (1.0 - decay_rate) * width_out / FF
    hidden_out, sum_out = lax.psum((jnp.sum(square_out, axis=1), jnp.sum(width_out)), "dp")
    rows_out = decay_rate * row_out + (1.0 - decay_rate) * hidden_out / D
    mean_out = (decay_rate * row_out_sum + (1.0 - decay_rate) * sum_out / D) / FF
    update_out = grad_out / jnp.sqrt(rows_out[:, None] * cols_out[None, :] / mean_out)
    new_master_out = master_out - step_size * update_out

    pre_grad_all, new_master_out, pieces = lax.optimization_barrier(
        (pre_grad_all, new_master_out, pieces)
    )
    input_grad = sum(piece.astype(jnp.float32) for piece in pieces).astype(jnp.bfloat16)
    grad_in = with_layout_constraint(contract_rows(in_cols, pre_grad_all), Layout((0, 1)))
    square_in = grad_in * grad_in + tiny_square
    width_in = lax.psum(jnp.sum(square_in, axis=1), "mp")
    rows_in = decay_rate * row_in + (1.0 - decay_rate) * width_in / FF
    hidden_in, sum_in = lax.psum((jnp.sum(square_in, axis=0), jnp.sum(rows_in)), "dp")
    cols_in = decay_rate * col_in + (1.0 - decay_rate) * hidden_in / D
    mean_in = sum_in / D
    update_in = grad_in / jnp.sqrt(rows_in[:, None] * cols_in[None, :] / mean_in)
    new_master_in = master_in - step_size * update_in
    return (input_grad, new_master_in, new_master_out)


MESH = pl.DeviceIdType.MESH
NT = (((1,), (1,)), ((), ()))
NN = (((1,), (0,)), ((), ()))
LANES = 128


def dot(left, right, dims):
    return lax.dot_general(left, right, dims, preferred_element_type=jnp.float32)


class Copies:
    def __init__(self, sems):
        self.sems = sems
        self.count = 0
        self.sent = []

    def take(self, number=1):
        first = self.count
        self.count += number
        return first

    def local(self, src, dst):
        copy = pltpu.make_async_copy(src, dst, self.sems.at[self.take()])
        copy.start()
        return copy

    def remote(self, src, dst, recv, **device):
        copy = pltpu.make_async_remote_copy(
            src_ref=src,
            dst_ref=dst,
            send_sem=self.sems.at[self.take()],
            recv_sem=self.sems.at[recv],
            device_id=device,
            device_id_type=MESH,
        )
        copy.start()
        self.sent.append(copy)

    def arrived(self, dst, recv, **device):
        pltpu.make_async_remote_copy(
            src_ref=dst,
            dst_ref=dst,
            send_sem=self.sems.at[recv],
            recv_sem=self.sems.at[recv],
            device_id=device,
            device_id_type=MESH,
        ).wait_recv()

    def drain(self):
        for copy in self.sent:
            copy.wait_send()


def step_kernel(
    plan,
    og_hbm, pa_hbm, in_hbm, wo_hbm, wi_hbm, row_out, col_out, row_in, col_in,
    ig_ref, go_hbm, gi_hbm, fro_ref, fco_ref, fri_ref, fci_ref,
    og2, pa2, hid, pre, oc, ic, ict, wob, wib, ipb, rpb, go, gi, racc,
    vec_d, vec_m, sems, local_sems,
):
    n_dp, n_mp, tok, width, ff, cols, parts = plan
    half, depth = ff // 2, width // 2
    piece = width // n_mp
    chunk = half // parts
    d, z = lax.axis_index("dp"), lax.axis_index("mp")
    core, chip = lax.rem(d, 2), d // 2
    base = pl.multiple_of(chip * 2 * tok, 2 * tok)
    flip = lambda index: d + sum(
        bit * (1 - 2 * lax.rem(d // bit, 2)) for bit in (1, 2, 4) if index & bit
    )
    turn = lambda index: z + sum(
        bit * (1 - 2 * lax.rem(z // bit, 2)) for bit in (1, 2) if index & bit
    )
    dp_of = {index: flip(index) for index in range(1, n_dp)}
    mp_of = {index: turn(index) for index in range(1, n_mp)}
    on = lambda index: dict(dp=dp_of[index], mp=z)

    barrier = pltpu.get_barrier_semaphore()
    for index in range(1, n_dp):
        pl.semaphore_signal(barrier, inc=1, device_id=on(index), device_id_type=MESH)
    for index in range(1, n_mp):
        for peer in (d, dp_of[1]):
            device = dict(dp=peer, mp=mp_of[index])
            pl.semaphore_signal(barrier, inc=1, device_id=device, device_id_type=MESH)

    c = Copies(sems)
    rows_of = lambda who: pl.ds(pl.multiple_of(who * tok, tok), tok)
    mine = pl.ds(pl.multiple_of(core * tok, tok), tok)
    other = pl.ds(pl.multiple_of((1 - core) * tok, tok), tok)
    half_cols = lambda which: pl.ds(pl.multiple_of(which * half, half), half)
    start = [
        c.local(pa_hbm.at[:, half_cols(core)], pa2.at[mine]),
        c.local(og_hbm, og2.at[mine]),
    ]
    own_cols = pl.ds(pl.multiple_of(d * cols, cols), cols)
    own_oc = c.local(og_hbm.at[:, own_cols], oc.at[rows_of(d)])
    own_ic = c.local(in_hbm.at[:, own_cols], ic.at[rows_of(d)])

    n_out = half // chunk
    slots = wob.shape[0]
    wo_copy = lambda k: pltpu.make_async_copy(
        wo_hbm.at[pl.ds(pl.multiple_of(core * half + k * chunk, chunk), chunk)],
        wob.at[k % slots],
        local_sems.at[k % slots],
    )
    in_rows = wib.shape[1]
    n_in = depth // in_rows
    wi_copy = lambda k: pltpu.make_async_copy(
        wi_hbm.at[pl.ds(pl.multiple_of(core * depth + k * in_rows, in_rows), in_rows)],
        wib.at[k % slots],
        local_sems.at[slots + k % slots],
    )
    for k in range(slots):
        wo_copy(k).start()

    pl.semaphore_wait(barrier, n_dp - 1 + 2 * (n_mp - 1))

    r_pa, r_og = c.take(), c.take()
    c.remote(pa_hbm.at[:, half_cols(1 - core)], pa2.at[mine], r_pa, **on(1))
    c.remote(og_hbm, og2.at[mine], r_og, **on(1))

    r_oc, r_ic = c.take(n_dp), c.take(n_dp)

    def spread(src, dst, recv):
        for index in (2, 4, 6, 3, 5, 7, 1):
            who = dp_of[index]
            their = pl.ds(pl.multiple_of(who * cols, cols), cols)
            c.remote(src.at[:, their], dst.at[rows_of(d)], recv + index, **on(index))

    def gathered(dst, recv):
        for index in range(1, n_dp):
            c.arrived(dst.at[rows_of(dp_of[index])], recv + index, **on(index))

    spread(og_hbm, oc, r_oc)

    def block(dst, index, which, k):
        tokens = pl.ds(pl.multiple_of((dp_of[index] if index else d) // 2 * 2 * tok, 2 * tok), 2 * tok)
        units = pl.ds(pl.multiple_of(which * half + k * chunk, chunk), chunk)
        return dst.at[units, tokens] if dst is hid else dst.at[tokens, units]

    r_h, r_p = {}, {}
    for table in (r_h, r_p):
        for index in (0, 2, 4, 6):
            table[index] = c.take(parts), c.take(parts)

    def send_own(dst, table, k):
        src = block(dst, 0, core, k)
        c.remote(src, src, table[2][0] + k, **on(2))
        c.remote(src, src, table[4][0] + k, **on(4))
        c.remote(src, src, table[0][1] + k, **on(1))

    def pass_on(dst, table, index, k):
        src = block(dst, index, core, k)
        c.arrived(src, table[index][0] + k, **on(index))
        if index == 2 and k < parts // 2:
            c.remote(src, src, table[6][0] + k, **on(4))
        if index == 4 and k >= parts // 2:
            c.remote(src, src, table[6][0] + k, **on(2))
        c.remote(src, src, table[index][1] + k, **on(1))

    def from_partner(dst, table, index, k):
        c.arrived(block(dst, index, 1 - core, k), table[index][1] + k, **on(1))

    for copy in start:
        copy.wait()
    c.arrived(pa2.at[other], r_pa, **on(1))

    for k in range(parts):
        units = slice(k * chunk, (k + 1) * chunk)
        active, _ = gelu_parts(pa2[:, units].astype(jnp.float32))
        target = pl.ds(pl.multiple_of(core * half + k * chunk, chunk), chunk)
        hid[target, pl.ds(base, 2 * tok)] = active.T.astype(jnp.bfloat16)
        if k:
            send_own(hid, r_h, k - 1)
    c.arrived(og2.at[other], r_og, **on(1))
    for k in range(n_in if n_in < slots else slots):
        wi_copy(k).start()
    for k in range(parts):
        wo_copy(k).wait()
        hid_grad = dot(og2[...], wob[k % slots], NT)
        _, slope = gelu_parts(pa2[:, k * chunk : (k + 1) * chunk].astype(jnp.float32))
        target = pl.ds(pl.multiple_of(core * half + k * chunk, chunk), chunk)
        pre[pl.ds(base, 2 * tok), target] = (hid_grad * slope).astype(jnp.bfloat16)
        if k + slots < n_out:
            wo_copy(k + slots).start()
        if k:
            send_own(pre, r_p, k - 1)
        else:
            send_own(hid, r_h, parts - 1)
            spread(in_hbm, ic, r_ic)
    for k in range(parts - 1):
        from_partner(pre, r_p, 0, k)
    send_own(pre, r_p, parts - 1)
    from_partner(pre, r_p, 0, parts - 1)

    r_rp = c.take(n_mp)
    owned = n_mp // 2
    s_rp = c.take(owned * 2)

    def piece_copy(which, t):
        to = core * owned + which
        return pltpu.make_async_remote_copy(
            src_ref=ipb.at[which, pl.ds(t * tok, tok)],
            dst_ref=rpb.at[z],
            send_sem=sems.at[s_rp + which * 2 + t],
            recv_sem=sems.at[r_rp + z],
            device_id=dict(dp=chip * 2 + t, mp=to),
            device_id_type=MESH,
        ), jnp.logical_or(to != z, core != t)

    def send_pieces(which):
        for t in range(2):
            copy, away = piece_copy(which, t)

            @pl.when(away)
            def _():
                copy.start()

    per = n_in // owned
    for k in range(n_in):
        wi_copy(k).wait()
        part = dot(pre[pl.ds(base, 2 * tok), :], wib[k % slots], NT)
        ipb[k // per, :, k % per * in_rows : (k % per + 1) * in_rows] = part.astype(jnp.bfloat16)
        if k + slots < n_in:
            wi_copy(k + slots).start()
        if k and k % per == 0:
            send_pieces(k // per - 1)

    own_ic.wait()
    own_oc.wait()
    gathered(oc, r_oc)
    send_pieces(owned - 1)

    for k in range(parts):
        pass_on(hid, r_h, 2, k)
        pass_on(hid, r_h, 4, k)
    gathered(ic, r_ic)
    ict[...] = ic[...].astype(jnp.float32).T.astype(jnp.bfloat16)
    for k in range(parts // 2):
        pass_on(hid, r_h, 6, k)
        pass_on(hid, r_h, 6, k + parts // 2)
    for k in range(parts):
        for index in (0, 2, 4, 6):
            from_partner(hid, r_h, index, k)

    def as_rows(row, ref, at):
        for j in range(row.shape[1] // LANES):
            ref[at + j : at + j + 1, :] = row[:, j * LANES : (j + 1) * LANES]

    out_rows = 2 * chunk
    written = []
    zero_m = jnp.zeros((vec_m.shape[1], LANES), jnp.float32)
    for slot in (0, 1):
        vec_m[slot * n_mp] = zero_m
    width_sum = jnp.zeros((1, cols), jnp.float32)
    for k in range(parts):
        rows = slice(k * out_rows, (k + 1) * out_rows)
        grad = dot(hid[rows, :], oc[...], NN)
        square = grad * grad + tiny_square
        width_sum += jnp.sum(square, axis=0, keepdims=True)
        lanes = sum(square[:, j * LANES : (j + 1) * LANES] for j in range(cols // LANES))
        as_rows(jnp.sum(lanes.T, axis=0, keepdims=True), vec_d.at[0], k * out_rows // LANES)
        go[rows, :] = grad.astype(jnp.bfloat16)
        if k:
            last = slice((k - 1) * out_rows, k * out_rows)
            written.append(c.local(go.at[last], go_hbm.at[last]))
        pass_on(pre, r_p, 2, k)
        pass_on(pre, r_p, 4, k)
    as_rows(width_sum, vec_m.at[0], 0)

    def exchange_d(slot, height):
        recv = c.take(n_dp)
        src = vec_d.at[slot * n_dp, pl.ds(0, height)]
        for index in range(1, n_dp):
            dst = vec_d.at[slot * n_dp + index, pl.ds(0, height)]
            c.remote(src, dst, recv + index, **on(index))

        def total():
            for index in range(1, n_dp):
                c.arrived(vec_d.at[slot * n_dp + index, pl.ds(0, height)], recv + index, **on(index))
            return sum(vec_d[slot * n_dp + index, :height] for index in range(n_dp))

        return total

    def exchange_m(slot):
        recv = c.take(n_mp)
        src = vec_m.at[slot * n_mp]
        for index in range(1, n_mp):
            device = dict(dp=d, mp=mp_of[index])
            c.remote(src, vec_m.at[slot * n_mp + index], recv + index, **device)

        def total():
            for index in range(1, n_mp):
                device = dict(dp=d, mp=mp_of[index])
                c.arrived(vec_m.at[slot * n_mp + index], recv + index, **device)
            return sum(vec_m[slot * n_mp + index] for index in range(n_mp))

        return total

    last = slice((parts - 1) * out_rows, parts * out_rows)
    written.append(c.local(go.at[last], go_hbm.at[last]))
    high = ff // LANES
    hidden_out = exchange_d(0, high)
    width_out = exchange_m(0)

    racc[...] = jnp.zeros_like(racc)

    def grad_in(which, k):
        units = pl.ds(pl.multiple_of(which * half + k * chunk, chunk), chunk)
        at = which * parts + k
        grad = dot(ict[...], pre[:, units], NN)
        square = grad * grad + tiny_square
        as_rows(jnp.sum(square, axis=0, keepdims=True), vec_d.at[n_dp], at * chunk // LANES)
        racc[...] += sum(square[:, j * LANES : (j + 1) * LANES] for j in range(chunk // LANES))
        gi[at] = grad.astype(jnp.bfloat16)
        return at, units

    def write_in(at, units):
        written.append(c.local(gi.at[at], gi_hbm.at[:, units]))

    pending = []
    for k in range(parts // 2):
        ready = (k, k + parts // 2)
        for j in ready:
            pass_on(pre, r_p, 6, j)
        if k == 0:
            total = decay_rate * row_out[...] + (1.0 - decay_rate) * hidden_out() / width
            rows_out = total
            vec_m[2 * n_mp] = jnp.broadcast_to(jnp.sum(total), (8, LANES))
            width_total = width_out()
            fco_ref[...] = lax.rsqrt(decay_rate * col_out[...] + (1.0 - decay_rate) * width_total / (ff * n_mp))
            for s in range(n_mp):
                gone = jnp.logical_or(s != z, core != z // owned)

                @pl.when(gone)
                def _():
                    c.arrived(rpb.at[s], r_rp + s, dp=chip * 2 + z // owned, mp=s)

            @pl.when(core == z // owned)
            def _():
                rpb[z] = ipb[z - core * owned, mine, :]

            ig_ref[...] = sum(rpb[s].astype(jnp.float32) for s in range(n_mp)).astype(jnp.bfloat16)
        for j in ready:
            for index in (2, 4, 6):
                from_partner(pre, r_p, index, j)
        if k == 0:
            sum_rows = exchange_m(2)
        for j in ready:
            for which in (0, 1):
                pending.append(grad_in(which, j))
        if k:
            for item in pending[:-4]:
                write_in(*item)
            pending = pending[-4:]
    as_rows(jnp.sum(racc[...].T, axis=0, keepdims=True), vec_m.at[n_mp], 0)
    for item in pending:
        write_in(*item)
    width_in = exchange_m(1)
    hidden_in = exchange_d(1, high)
    mean_out = sum_rows() / (ff * n_mp)
    fro_ref[...] = step_size * lax.rsqrt(rows_out / mean_out[0:1, :])
    rows_in = decay_rate * row_in[...] + (1.0 - decay_rate) * width_in() / (ff * n_mp)
    vec_d[2 * n_dp, :8] = jnp.broadcast_to(jnp.sum(rows_in), (8, LANES))
    fci_ref[...] = lax.rsqrt(decay_rate * col_in[...] + (1.0 - decay_rate) * hidden_in() / width)
    mean_in = exchange_d(2, 8)() / width
    fri_ref[...] = step_size * lax.rsqrt(rows_in / mean_in[0:1, :])
    for which in range(owned):
        for t in range(2):
            copy, away = piece_copy(which, t)

            @pl.when(away)
            def _():
                copy.wait_send()

    c.drain()
    for copy in written:
        copy.wait()


def fast_body(n_dp, n_mp, inputs, pre_act, out_grad, w_in, w_out, master_in, master_out, row_in, col_in, row_out, col_out):
    tok, width = inputs.shape
    ff = pre_act.shape[1]
    cols = width // n_dp
    parts = PARTS
    chunk = ff // 2 // parts
    in_rows = 2 * chunk
    high, low = ff // LANES, cols // LANES
    pad = (-low) % 8
    as_tile = lambda v: jnp.pad(v.reshape(low, LANES), ((0, pad), (0, 0)))
    slots = 3
    bf, f32 = jnp.bfloat16, jnp.float32
    anywhere = pl.BlockSpec(memory_space=pl.ANY)
    vmem = pl.BlockSpec(memory_space=pltpu.VMEM)
    shape = jax.ShapeDtypeStruct
    plan = (n_dp, n_mp, tok, width, ff, cols, parts)
    ig, go, gi, fro, fco, fri, fci = pl.pallas_call(
        functools.partial(step_kernel, plan),
        out_shape=(
            shape((tok, width // n_mp), bf),
            shape((ff, cols), bf),
            shape((cols, ff), bf),
            shape((high, LANES), f32),
            shape((low + pad, LANES), f32),
            shape((low + pad, LANES), f32),
            shape((high, LANES), f32),
        ),
        in_specs=[anywhere] * 5 + [vmem] * 4,
        out_specs=(vmem, anywhere, anywhere, vmem, vmem, vmem, vmem),
        scratch_shapes=[
            pltpu.VMEM((2 * tok, width), bf),
            pltpu.VMEM((2 * tok, ff // 2), bf),
            pltpu.VMEM((ff, n_dp * tok), bf),
            pltpu.VMEM((n_dp * tok, ff), bf),
            pltpu.VMEM((n_dp * tok, cols), bf),
            pltpu.VMEM((n_dp * tok, cols), bf),
            pltpu.VMEM((cols, n_dp * tok), bf),
            pltpu.VMEM((slots, chunk, width), bf),
            pltpu.VMEM((slots, in_rows, ff), bf),
            pltpu.VMEM((n_mp // 2, 2 * tok, width // n_mp), bf),
            pltpu.VMEM((n_mp, tok, width // n_mp), bf),
            pltpu.VMEM((ff, cols), bf),
            pltpu.VMEM((2 * parts, cols, chunk), bf),
            pltpu.VMEM((cols, LANES), f32),
            pltpu.VMEM((3 * n_dp, high, LANES), f32),
            pltpu.VMEM((3 * n_mp, low + pad, LANES), f32),
            pltpu.SemaphoreType.DMA((420,)),
            pltpu.SemaphoreType.DMA((2 * slots,)),
        ],
        compiler_params=pltpu.CompilerParams(
            collective_id=0, has_side_effects=True, vmem_limit_bytes=64 * 2**20 - 2**16
        ),
    )(
        out_grad, pre_act, inputs, w_out, w_in,
        row_out.reshape(high, LANES), as_tile(col_out), as_tile(row_in), col_in.reshape(high, LANES),
    )
    flat = lambda t, n: t.reshape(-1)[:n]
    new_master_out = master_out - go.astype(f32) * flat(fro, ff)[:, None] * flat(fco, cols)[None, :]
    new_master_in = master_in - gi.astype(f32) * flat(fri, cols)[:, None] * flat(fci, ff)[None, :]
    return ig, new_master_in, new_master_out


PARTS = 6


def fits(mesh):
    n_dp, n_mp = mesh.shape["dp"], mesh.shape["mp"]
    return n_dp == 8 and n_mp == 4 and D % (n_dp * LANES) == 0 and FF % (n_mp * 2 * PARTS * LANES) == 0


def solution(mesh):
    in_specs = (
        P("dp", None),
        P("dp", "mp"),
        P("dp", None),
        P(None, "mp"),
        P("mp", None),
        P("dp", "mp"),
        P("mp", "dp"),
        P("dp"),
        P("mp"),
        P("mp"),
        P("dp"),
    )
    out_specs = (P("dp", "mp"), P("dp", "mp"), P("mp", "dp"))
    run = body
    if fits(mesh):
        run = functools.partial(fast_body, mesh.shape["dp"], mesh.shape["mp"])
    return jax.shard_map(run, mesh=mesh, in_specs=in_specs, out_specs=out_specs, check_vma=False)
```

```python
import functools
import math

import jax
import jax.numpy as jnp
from jax import lax
from jax.experimental import pallas as pl
from jax.experimental.pallas import tpu as pltpu
from jax.experimental.layout import Layout, with_layout_constraint
from jax.sharding import PartitionSpec as P

D = 6144
FF = 12288


decay_rate = 0.8
step_size = 0.05
tiny_square = 1e-30


def gelu_parts(pre):
    cumulative = 0.5 * (1.0 + jax.scipy.special.erf(pre * (1.0 / math.sqrt(2.0))))
    density = jnp.exp(-0.5 * pre * pre) * (1.0 / math.sqrt(2.0 * math.pi))
    return (pre * cumulative, cumulative + pre * density)


def contract_rows(left, right):
    return lax.dot_general(
        left, right, (((0,), (0,)), ((), ())), preferred_element_type=jnp.float32
    )


def scatter_pieces(partial, axis):
    size = lax.axis_size(axis)
    me = lax.axis_index(axis)
    width = partial.shape[1] // size
    piece = lambda k: lax.dynamic_slice_in_dim(partial, k * width, width, 1)
    pieces = [piece(me)]
    for shift in range(1, size):
        moved = piece(lax.rem(me + shift, size)).astype(jnp.bfloat16)
        pieces.append(lax.ppermute(moved, axis, [(i, (i + shift) % size) for i in range(size)]))
    return pieces


def body(
    inputs, pre_act, out_grad, w_in, w_out, master_in, master_out, row_in, col_in, row_out, col_out
):
    active, slope = gelu_parts(pre_act.astype(jnp.float32))
    hidden = active.astype(jnp.bfloat16)
    hidden_all = lax.all_gather(hidden, "dp", axis=0, tiled=True)
    out_grad, _ = lax.optimization_barrier((out_grad, hidden))
    out_cols = lax.all_to_all(out_grad, "dp", 1, 0, tiled=True)
    hid_grad = lax.dot_general(
        out_grad, w_out, (((1,), (1,)), ((), ())), preferred_element_type=jnp.float32
    )
    pre_grad = (hid_grad * slope).astype(jnp.bfloat16)
    pre_grad_all = lax.all_gather(pre_grad, "dp", axis=0, tiled=True)
    input_part = lax.dot_general(
        pre_grad, w_in, (((1,), (1,)), ((), ())), preferred_element_type=jnp.float32
    )
    inputs, input_part = lax.optimization_barrier((inputs, input_part))
    in_cols = lax.all_to_all(inputs, "dp", 1, 0, tiled=True)
    pieces = scatter_pieces(input_part, "mp")

    grad_out = contract_rows(hidden_all, out_cols)
    square_out = grad_out * grad_out + tiny_square
    width_out, row_out_sum = lax.psum((jnp.sum(square_out, axis=0), jnp.sum(row_out)), "mp")
    cols_out = decay_rate * col_out + (1.0 - decay_rate) * width_out / FF
    hidden_out, sum_out = lax.psum((jnp.sum(square_out, axis=1), jnp.sum(width_out)), "dp")
    rows_out = decay_rate * row_out + (1.0 - decay_rate) * hidden_out / D
    mean_out = (decay_rate * row_out_sum + (1.0 - decay_rate) * sum_out / D) / FF
    update_out = grad_out / jnp.sqrt(rows_out[:, None] * cols_out[None, :] / mean_out)
    new_master_out = master_out - step_size * update_out

    pre_grad_all, new_master_out, pieces = lax.optimization_barrier(
        (pre_grad_all, new_master_out, pieces)
    )
    input_grad = sum(piece.astype(jnp.float32) for piece in pieces).astype(jnp.bfloat16)
    grad_in = with_layout_constraint(contract_rows(in_cols, pre_grad_all), Layout((0, 1)))
    square_in = grad_in * grad_in + tiny_square
    width_in = lax.psum(jnp.sum(square_in, axis=1), "mp")
    rows_in = decay_rate * row_in + (1.0 - decay_rate) * width_in / FF
    hidden_in, sum_in = lax.psum((jnp.sum(square_in, axis=0), jnp.sum(rows_in)), "dp")
    cols_in = decay_rate * col_in + (1.0 - decay_rate) * hidden_in / D
    mean_in = sum_in / D
    update_in = grad_in / jnp.sqrt(rows_in[:, None] * cols_in[None, :] / mean_in)
    new_master_in = master_in - step_size * update_in
    return (input_grad, new_master_in, new_master_out)


MESH = pl.DeviceIdType.MESH
NT = (((1,), (1,)), ((), ()))
NN = (((1,), (0,)), ((), ()))
LANES = 128


def dot(left, right, dims):
    return lax.dot_general(left, right, dims, preferred_element_type=jnp.float32)


class Copies:
    def __init__(self, sems, away):
        self.sems = sems
        self.away = away
        self.count = 0
        self.sent = []

    def take(self, number=None):
        first = self.count
        self.count += number or 1
        assert self.count <= SEMAPHORES
        return first if number is None else range(first, self.count)

    def local(self, src, dst, sem):
        pltpu.make_async_copy(src, dst, self.sems.at[sem]).start()

    def settled(self, region, sem):
        pltpu.make_async_copy(region, region, self.sems.at[sem]).wait()

    def sends(self, *regions):
        sem = self.take()
        self.sent += [(region, sem) for region in regions]
        return sem

    def moved(self, src, dst, send, recv, device):
        return pltpu.make_async_remote_copy(
            src_ref=src,
            dst_ref=dst,
            send_sem=self.sems.at[send],
            recv_sem=self.sems.at[recv],
            device_id=device,
            device_id_type=MESH,
        )

    def remote(self, src, dst, send, recv, **device):
        self.moved(src, dst, send, recv, device).start()

    def arrived(self, region, recv):
        self.moved(region, region, recv, recv, self.away).wait_recv()

    def drain(self):
        for region, sem in self.sent:
            self.moved(region, region, sem, sem, self.away).wait_send()


def step_kernel(
    plan,
    og_hbm, pa_hbm, in_hbm, wo_hbm, wi_hbm, ro_hbm, co_hbm, ri_hbm, ci_hbm,
    ig_hbm, go, gi, fac,
    og2, pa2, hid, pre, oc, ic, ict, wb, ipb, rpb, racc, vec_d, vec_m, igb,
    row_out, col_out, row_in, col_in, sems,
):
    n_dp, n_mp, tok, width, ff, cols, parts = plan
    half, depth = ff // 2, width // 2
    piece = width // n_mp
    chunk = half // parts
    d, z = lax.axis_index("dp"), lax.axis_index("mp")
    core, chip = lax.rem(d, 2), d // 2
    base = pl.multiple_of(chip * 2 * tok, 2 * tok)
    flip = lambda index: d + sum(
        bit * (1 - 2 * lax.rem(d // bit, 2)) for bit in (1, 2, 4) if index & bit
    )
    turn = lambda index: z + sum(
        bit * (1 - 2 * lax.rem(z // bit, 2)) for bit in (1, 2) if index & bit
    )
    dp_of = {index: flip(index) for index in range(1, n_dp)}
    mp_of = {index: turn(index) for index in range(1, n_mp)}
    on = lambda index: dict(dp=dp_of[index], mp=z)

    barrier = pltpu.get_barrier_semaphore()
    for index in range(1, n_dp):
        pl.semaphore_signal(barrier, inc=1, device_id=on(index), device_id_type=MESH)
    for index in range(1, n_mp):
        for peer in (d, dp_of[1]):
            device = dict(dp=peer, mp=mp_of[index])
            pl.semaphore_signal(barrier, inc=1, device_id=device, device_id_type=MESH)

    c = Copies(sems, on(1))
    rows_of = lambda who: pl.ds(pl.multiple_of(who * tok, tok), tok)
    mine = pl.ds(pl.multiple_of(core * tok, tok), tok)
    other = pl.ds(pl.multiple_of((1 - core) * tok, tok), tok)
    half_cols = lambda which: pl.ds(pl.multiple_of(which * half, half), half)
    l_pa, l_og, l_oc, l_ic, l_ig = (c.take() for _ in range(5))
    own_cols = pl.ds(pl.multiple_of(d * cols, cols), cols)
    c.local(pa_hbm.at[:, half_cols(core)], pa2.at[mine], l_pa)
    c.local(og_hbm, og2.at[mine], l_og)

    side = width // ff
    slots = wb.shape[0]
    in_rows = side * chunk
    n_out, n_in = half // chunk, depth // in_rows
    w_sems = c.take(slots)[0]

    def fetch(item):
        slot = item % slots
        if item < n_out:
            rows = pl.ds(pl.multiple_of(core * half + item * chunk, chunk), chunk)
            c.local(wo_hbm.at[rows], wb.at[slot], w_sems + slot)
        elif item < n_out + n_in:
            for part in range(side):
                at = core * depth + (item - n_out) * in_rows + part * chunk
                rows = pl.ds(pl.multiple_of(at, chunk), chunk)
                to = wb.at[slot, :, pl.ds(part * ff, ff)]
                c.local(wi_hbm.at[rows], to, w_sems + slot)

    fetched = lambda item: c.settled(wb.at[item % slots], w_sems + item % slots)
    for item in range(slots):
        fetch(item)
    c.local(og_hbm.at[:, own_cols], oc.at[rows_of(d)], l_oc)
    c.local(in_hbm.at[:, own_cols], ic.at[rows_of(d)], l_ic)
    vectors = ((ro_hbm, row_out), (co_hbm, col_out), (ri_hbm, row_in), (ci_hbm, col_in))
    l_vectors = c.take(4)
    for (src, dst), sem in zip(vectors, l_vectors):
        c.local(src, dst, sem)

    pl.semaphore_wait(barrier, n_dp - 1 + 2 * (n_mp - 1))

    even = lax.rem(z, 2)
    part_rows = lambda who, which: pl.ds(
        pl.multiple_of(who * tok + which * (tok // 2), tok // 2), tok // 2
    )
    beside = dict(dp=d, mp=mp_of[1])

    def spread(src, dst):
        near, beyond, partner = c.take(3)
        send = c.sends(dst.at[pl.ds(0, (n_dp - 1) * tok)])
        for index in (2, 4, 6, 3, 5, 7):
            their = pl.ds(pl.multiple_of(dp_of[index] * cols, cols), cols)
            c.remote(src.at[part_rows(0, even), their], dst.at[part_rows(d, even)], send, near, **on(index))
        their = pl.ds(pl.multiple_of(dp_of[1] * cols, cols), cols)
        c.remote(src.at[:, their], dst.at[rows_of(d)], send, partner, **on(1))

        def hand_on():
            c.arrived(dst.at[pl.ds(0, (n_dp - 2) * (tok // 2))], near)
            for index in range(2, n_dp):
                rows = dst.at[part_rows(dp_of[index], even)]
                c.remote(rows, rows, send, beyond, **beside)

        def gathered():
            c.arrived(dst.at[rows_of(dp_of[1])], partner)
            c.arrived(dst.at[pl.ds(0, (n_dp - 2) * (tok // 2))], beyond)

        return hand_on, gathered

    hand_on_oc, gathered_oc = spread(og_hbm, oc)
    r_pa, r_og = c.take(2)
    c.remote(
        pa_hbm.at[:, half_cols(1 - core)], pa2.at[mine], c.sends(pa2.at[mine]), r_pa, **on(1)
    )
    c.remote(og_hbm, og2.at[mine], c.sends(og2.at[mine]), r_og, **on(1))
    hand_on_ic, gathered_ic = spread(in_hbm, ic)

    def block(dst, index, which, k):
        tokens = pl.ds(pl.multiple_of((dp_of[index] if index else d) // 2 * 2 * tok, 2 * tok), 2 * tok)
        units = pl.ds(pl.multiple_of(which * half + k * chunk, chunk), chunk)
        return dst.at[units, tokens] if dst is hid else dst.at[tokens, units]

    class Stream:
        def __init__(self, dst):
            self.dst = dst
            self.near = {index: c.take(parts) for index in (2, 4, 6)}
            self.pairs = {index: c.take() for index in (0, 2, 4)}
            self.pairs[6] = c.take(parts)
            units, tokens = pl.ds(0, parts // 2 * 3 * chunk), pl.ds(0, 2 * tok)
            some = dst.at[units, tokens] if dst is hid else dst.at[tokens, units]
            whole = pl.ds(0, n_dp // 2 * tok)
            most = dst.at[:, whole] if dst is hid else dst.at[whole, :]
            self.send = {2: c.sends(some), 4: c.sends(some), 1: c.sends(most)}

        def across(self, index, k):
            return self.pairs[6][k] if index == 6 else self.pairs[index]

        def own(self, k, index):
            src = block(self.dst, 0, core, k)
            recv = self.pairs[0] if index == 1 else self.near[index][k]
            c.remote(src, src, self.send[index], recv, **on(index))

        def pass_on(self, index, k):
            src = block(self.dst, index, core, k)
            c.arrived(src, self.near[index][k])
            if index == 2 and k < parts // 2:
                c.remote(src, src, self.send[4], self.near[6][k], **on(4))
            if index == 4 and k >= parts // 2:
                c.remote(src, src, self.send[2], self.near[6][k], **on(2))
            c.remote(src, src, self.send[1], self.across(index, k), **on(1))

        def whole_from_partner(self, index):
            tokens = pl.ds(pl.multiple_of((dp_of[index] if index else d) // 2 * 2 * tok, 2 * tok), 2 * tok)
            units = half_cols(1 - core)
            region = self.dst.at[units, tokens] if self.dst is hid else self.dst.at[tokens, units]
            c.arrived(region, self.pairs[index])

        def diagonal_from_partner(self, k):
            c.arrived(block(self.dst, 6, 1 - core, k), self.pairs[6][k])

    h_flow, p_flow = Stream(hid), Stream(pre)
    c.settled(pa2.at[mine], l_pa)
    c.arrived(pa2.at[other], r_pa)

    for k in range(parts):
        units = slice(k * chunk, (k + 1) * chunk)
        active, _ = gelu_parts(pa2[:, units].astype(jnp.float32))
        target = pl.ds(pl.multiple_of(core * half + k * chunk, chunk), chunk)
        hid[target, pl.ds(base, 2 * tok)] = active.T.astype(jnp.bfloat16)
        if k:
            for index in (2, 4, 1):
                h_flow.own(k - 1, index)
    c.settled(og2.at[mine], l_og)
    c.arrived(og2.at[other], r_og)
    for k in range(parts):
        fetched(k)
        hid_grad = dot(og2[...], wb[k % slots], NT)
        _, slope = gelu_parts(pa2[:, k * chunk : (k + 1) * chunk].astype(jnp.float32))
        target = pl.ds(pl.multiple_of(core * half + k * chunk, chunk), chunk)
        pre[pl.ds(base, 2 * tok), target] = (hid_grad * slope).astype(jnp.bfloat16)
        fetch(k + slots)
        if k:
            p_flow.own(k - 1, 1)
        else:
            for index in (2, 4, 1):
                h_flow.own(parts - 1, index)
    hand_on_oc()
    p_flow.own(parts - 1, 1)
    p_flow.whole_from_partner(0)

    r_rp = c.take(n_mp)[0]
    owned = n_mp // 2
    s_rp = c.take(owned * 2)[0]

    def piece_copy(which, t):
        to = core * owned + which
        return pltpu.make_async_remote_copy(
            src_ref=ipb.at[which, pl.ds(t * tok, tok)],
            dst_ref=rpb.at[z],
            send_sem=sems.at[s_rp + which * 2 + t],
            recv_sem=sems.at[r_rp + z],
            device_id=dict(dp=chip * 2 + t, mp=to),
            device_id_type=MESH,
        ), jnp.logical_or(to != z, core != t)

    def send_pieces(which):
        for t in range(2):
            copy, away = piece_copy(which, t)

            @pl.when(away)
            def _():
                copy.start()

    per = n_in // owned
    for k in range(n_in):
        item = n_out + k
        fetched(item)
        for part in range(side):
            rows = wb[item % slots, :, part * ff : (part + 1) * ff]
            value = dot(pre[pl.ds(base, 2 * tok), :], rows, NT).astype(jnp.bfloat16)
            at = k % per * in_rows + part * chunk
            ipb[k // per, :, at : at + chunk] = value
        fetch(item + slots)
    hand_on_ic()
    for which in range(owned):
        send_pieces(which)

    for k in range(parts):
        h_flow.pass_on(2, k)
        h_flow.pass_on(4, k)
        if k == parts // 2 - 1:
            for j in range(parts):
                p_flow.own(j, 4)
    for k in range(parts):
        p_flow.own(k, 2)
    for (_, dst), sem in zip(vectors, l_vectors):
        c.settled(dst, sem)
    c.settled(oc.at[rows_of(d)], l_oc)
    c.settled(ic.at[rows_of(d)], l_ic)
    for k in range(parts // 2):
        h_flow.pass_on(6, k)
        h_flow.pass_on(6, k + parts // 2)
    gathered_ic()
    ict[...] = ic[...].astype(jnp.float32).T.astype(jnp.bfloat16)
    gathered_oc()
    for index in (0, 2, 4):
        h_flow.whole_from_partner(index)
    for k in range(parts):
        h_flow.diagonal_from_partner(k)

    def as_rows(row, ref, at):
        for j in range(row.shape[1] // LANES):
            ref[pl.ds(at + j, 1), :] = row[:, j * LANES : (j + 1) * LANES]

    out_rows = 2 * chunk
    fac[...] = jnp.zeros_like(fac)
    zero_m = jnp.zeros((vec_m.shape[1], LANES), jnp.float32)
    for slot in (0, 1):
        vec_m[slot * n_mp] = zero_m
    width_sum = jnp.zeros((1, cols), jnp.float32)
    for k in range(parts):
        rows = slice(k * out_rows, (k + 1) * out_rows)
        grad = dot(hid[rows, :], oc[...], NN)
        square = grad * grad + tiny_square
        width_sum += jnp.sum(square, axis=0, keepdims=True)
        lanes = sum(square[:, j * LANES : (j + 1) * LANES] for j in range(cols // LANES))
        as_rows(jnp.sum(lanes.T, axis=0, keepdims=True), vec_d.at[0], k * out_rows // LANES)
        go[rows, :] = grad.astype(jnp.bfloat16)
        p_flow.pass_on(2, k)
        p_flow.pass_on(4, k)
    as_rows(width_sum, vec_m.at[0], 0)

    def exchange(table, slot, peers, height):
        recv = c.take()
        first = slot * (len(peers) + 1)
        rows = pl.ds(0, height)
        there = table.at[pl.ds(first + 1, len(peers)), rows]
        send = c.sends(there)
        for at, device in enumerate(peers):
            c.remote(table.at[first, rows], table.at[first + 1 + at, rows], send, recv, **device)

        def total():
            c.arrived(there, recv)
            return sum(table[first + at, :height] for at in range(len(peers) + 1))

        return total

    dp_peers = [on(index) for index in range(1, n_dp)]
    mp_peers = [dict(dp=d, mp=mp_of[index]) for index in range(1, n_mp)]
    exchange_d = lambda slot, height: exchange(vec_d, slot, dp_peers, height)
    exchange_m = lambda slot: exchange(vec_m, slot, mp_peers, vec_m.shape[1])
    high = ff // LANES
    hidden_out = exchange_d(0, high)
    width_out = exchange_m(0)

    racc[...] = jnp.zeros_like(racc)

    def grad_in(which, k):
        units = pl.ds(pl.multiple_of(which * half + k * chunk, chunk), chunk)
        at = which * parts + k
        grad = dot(ict[...], pre[:, units], NN)
        square = grad * grad + tiny_square
        as_rows(jnp.sum(square, axis=0, keepdims=True), vec_d.at[n_dp], at * chunk // LANES)
        racc[...] += sum(square[:, j * LANES : (j + 1) * LANES] for j in range(chunk // LANES))
        gi[:, units] = grad.astype(jnp.bfloat16)

    for index in (2, 4):
        p_flow.whole_from_partner(index)
    for k in range(parts // 2):
        ready = (k, k + parts // 2)
        for j in ready:
            p_flow.pass_on(6, j)
        for j in ready:
            grad_in(core, j)
        for j in ready:
            p_flow.diagonal_from_partner(j)
        for j in ready:
            grad_in(1 - core, j)
    as_rows(jnp.sum(racc[...].T, axis=0, keepdims=True), vec_m.at[n_mp], 0)
    width_in = exchange_m(1)
    hidden_in = exchange_d(1, high)
    low = cols // LANES
    rows_out = decay_rate * row_out[...] + (1.0 - decay_rate) * hidden_out() / width
    vec_m[2 * n_mp] = jnp.broadcast_to(jnp.sum(rows_out), vec_m.shape[1:])
    cols_out = decay_rate * col_out[...] + (1.0 - decay_rate) * width_out()[:low] / (ff * n_mp)
    for s in range(n_mp):
        gone = jnp.logical_or(s != z, core != z // owned)

        @pl.when(gone)
        def _():
            c.arrived(rpb.at[s], r_rp + s)

    sum_rows = exchange_m(2)

    @pl.when(core == z // owned)
    def _():
        rpb[z] = ipb[z - core * owned, mine, :]

    rows_in = decay_rate * row_in[...] + (1.0 - decay_rate) * width_in()[:low] / (ff * n_mp)
    vec_d[2 * n_dp, :8] = jnp.broadcast_to(jnp.sum(rows_in), (8, LANES))
    igb[...] = sum(rpb[s].astype(jnp.float32) for s in range(n_mp)).astype(jnp.bfloat16)
    sum_rows_in = exchange_d(2, 8)
    c.local(igb, ig_hbm, l_ig)
    fac[high : 2 * high] = lax.rsqrt(
        decay_rate * col_in[...] + (1.0 - decay_rate) * hidden_in() / width
    )
    fac[2 * high : 2 * high + low] = lax.rsqrt(cols_out)
    mean_out = sum_rows() / (ff * n_mp)
    fac[:high] = step_size * lax.rsqrt(rows_out / mean_out[0:1, :])
    mean_in = sum_rows_in() / width
    fac[2 * high + 8 : 2 * high + 8 + low] = step_size * lax.rsqrt(rows_in / mean_in[0:1, :])
    c.settled(igb, l_ig)
    for which in range(owned):
        for t in range(2):
            copy, away = piece_copy(which, t)

            @pl.when(away)
            def _():
                copy.wait_send()

    c.drain()


def update_kernel(plan, mo, mi_hbm, go, gi, fac, new_out, new_in, out_b, in_b, sems):
    ff, cols, tiles = plan
    high, low = ff // LANES, cols // LANES
    work = []
    for new, old, stage, grad, first, height, across, rows_at, cols_at in (
        (new_out, mo, out_b, go, 0, high, low, 0, 2 * high),
        (new_in, in_b, in_b, gi, tiles, low, high, 2 * high + 8, high),
    ):
        for tile in range(tiles):
            bands = range(tile * height // tiles, (tile + 1) * height // tiles)
            rows = slice(bands[0] * LANES, (bands[-1] + 1) * LANES)
            fetch = None
            if old is stage:
                fetch = pltpu.make_async_copy(mi_hbm.at[rows], stage.at[rows], sems.at[0, tile])
                fetch.start()
            store = pltpu.make_async_copy(stage.at[rows], new.at[rows], sems.at[1, first + tile])
            work.append((fetch, store, old, stage, grad, bands, across, rows_at, cols_at))
    turned = fac[...].T
    for fetch, store, old, stage, grad, bands, across, rows_at, cols_at in work:
        if fetch is not None:
            fetch.wait()
        for band in bands:
            rows = slice(band * LANES, (band + 1) * LANES)
            down = jnp.broadcast_to(turned[:, rows_at + band : rows_at + band + 1], (LANES, LANES))

            def lane_group(j, carry):
                at = pl.ds(pl.multiple_of(j * LANES, LANES), LANES)
                scale = down * fac[pl.ds(cols_at + j, 1), :]
                stage[rows, at] = old[rows, at] - grad[rows, at].astype(jnp.float32) * scale
                return carry

            lax.fori_loop(0, across, lane_group, 0, unroll=6)
        store.start()
    for _, store, *_ in work:
        store.wait()


def fast_body(n_dp, n_mp, inputs, pre_act, out_grad, w_in, w_out, master_in, master_out, row_in, col_in, row_out, col_out):
    tok, width = inputs.shape
    ff = pre_act.shape[1]
    cols = width // n_dp
    parts = PARTS
    chunk = ff // 2 // parts
    high, low = ff // LANES, cols // LANES
    slots, tiles = 2, math.gcd(high, low)
    bf, f32 = jnp.bfloat16, jnp.float32
    anywhere = pl.BlockSpec(memory_space=pl.ANY)
    vmem = pl.BlockSpec(memory_space=pltpu.VMEM)
    shape = jax.ShapeDtypeStruct
    plan = (n_dp, n_mp, tok, width, ff, cols, parts)
    in_hbm = lambda array: pltpu.with_memory_space_constraint(array, pltpu.HBM)
    in_vmem = lambda array: pltpu.with_memory_space_constraint(array, pltpu.VMEM)
    ig, *held = pl.pallas_call(
        functools.partial(step_kernel, plan),
        out_shape=(
            shape((tok, width // n_mp), bf),
            pltpu.VMEM((ff, cols), bf),
            pltpu.VMEM((cols, ff), bf),
            pltpu.VMEM((2 * high + 16, LANES), f32),
        ),
        in_specs=[anywhere] * 9,
        out_specs=(anywhere,) + (vmem,) * 3,
        scratch_shapes=[
            pltpu.VMEM((2 * tok, width), bf),
            pltpu.VMEM((2 * tok, ff // 2), bf),
            pltpu.VMEM((ff, n_dp * tok), bf),
            pltpu.VMEM((n_dp * tok, ff), bf),
            pltpu.VMEM((n_dp * tok, cols), bf),
            pltpu.VMEM((n_dp * tok, cols), bf),
            pltpu.VMEM((cols, n_dp * tok), bf),
            pltpu.VMEM((slots, chunk, width), bf),
            pltpu.VMEM((n_mp // 2, 2 * tok, width // n_mp), bf),
            pltpu.VMEM((n_mp, tok, width // n_mp), bf),
            pltpu.VMEM((cols, LANES), f32),
            pltpu.VMEM((3 * n_dp, high, LANES), f32),
            pltpu.VMEM((3 * n_mp, 8, LANES), f32),
            pltpu.VMEM((tok, width // n_mp), bf),
            pltpu.VMEM((high, LANES), f32),
            pltpu.VMEM((low, LANES), f32),
            pltpu.VMEM((low, LANES), f32),
            pltpu.VMEM((high, LANES), f32),
            pltpu.SemaphoreType.DMA((SEMAPHORES,)),
        ],
        compiler_params=pltpu.CompilerParams(
            collective_id=0, has_side_effects=True, vmem_limit_bytes=K1_VMEM
        ),
    )(
        *map(
            in_hbm,
            (
                out_grad, pre_act, inputs, w_out, w_in,
                row_out.reshape(high, LANES), col_out.reshape(low, LANES),
                row_in.reshape(low, LANES), col_in.reshape(high, LANES),
            ),
        )
    )
    new_master_out, new_master_in = pl.pallas_call(
        functools.partial(update_kernel, (ff, cols, tiles)),
        out_shape=(shape((ff, cols), f32), shape((cols, ff), f32)),
        in_specs=[vmem, anywhere, vmem, vmem, vmem],
        out_specs=(anywhere,) * 2,
        scratch_shapes=[
            pltpu.VMEM((ff, cols), f32),
            pltpu.VMEM((cols, ff), f32),
            pltpu.SemaphoreType.DMA((2, 2 * tiles)),
        ],
        compiler_params=pltpu.CompilerParams(vmem_limit_bytes=K2_VMEM),
    )(in_vmem(master_out), in_hbm(master_in), *map(in_vmem, held))
    return ig, new_master_in, new_master_out


SEMAPHORES = 110
K1_VMEM = 34 * 2**20
K2_VMEM = 21 * 2**20
PARTS = 6


def fits(mesh):
    n_dp, n_mp = mesh.shape["dp"], mesh.shape["mp"]
    return n_dp == 8 and n_mp == 4 and D % (n_dp * LANES) == 0 and D <= 8 * n_dp * LANES and D * n_mp % FF == 0 and FF % (n_mp * 2 * PARTS * LANES) == 0


def solution(mesh):
    in_specs = (
        P("dp", None),
        P("dp", "mp"),
        P("dp", None),
        P(None, "mp"),
        P("mp", None),
        P("dp", "mp"),
        P("mp", "dp"),
        P("dp"),
        P("mp"),
        P("mp"),
        P("dp"),
    )
    out_specs = (P("dp", "mp"), P("dp", "mp"), P("mp", "dp"))
    run = body
    if fits(mesh):
        run = functools.partial(fast_body, mesh.shape["dp"], mesh.shape["mp"])
    return jax.shard_map(run, mesh=mesh, in_specs=in_specs, out_specs=out_specs, check_vma=False)
```

```python
import functools
import math

import jax
import jax.numpy as jnp
from jax import lax
from jax.experimental import pallas as pl
from jax.experimental.pallas import tpu as pltpu
from jax.experimental.layout import Layout, with_layout_constraint
from jax.sharding import PartitionSpec as P

D = 6144
FF = 12288


decay_rate = 0.8
step_size = 0.05
tiny_square = 1e-30


def gelu_parts(pre):
    cumulative = 0.5 * (1.0 + jax.scipy.special.erf(pre * (1.0 / math.sqrt(2.0))))
    density = jnp.exp(-0.5 * pre * pre) * (1.0 / math.sqrt(2.0 * math.pi))
    return (pre * cumulative, cumulative + pre * density)


def contract_rows(left, right):
    return lax.dot_general(
        left, right, (((0,), (0,)), ((), ())), preferred_element_type=jnp.float32
    )


def scatter_pieces(partial, axis):
    size = lax.axis_size(axis)
    me = lax.axis_index(axis)
    width = partial.shape[1] // size
    piece = lambda k: lax.dynamic_slice_in_dim(partial, k * width, width, 1)
    pieces = [piece(me)]
    for shift in range(1, size):
        moved = piece(lax.rem(me + shift, size)).astype(jnp.bfloat16)
        pieces.append(lax.ppermute(moved, axis, [(i, (i + shift) % size) for i in range(size)]))
    return pieces


def body(
    inputs, pre_act, out_grad, w_in, w_out, master_in, master_out, row_in, col_in, row_out, col_out
):
    active, slope = gelu_parts(pre_act.astype(jnp.float32))
    hidden = active.astype(jnp.bfloat16)
    hidden_all = lax.all_gather(hidden, "dp", axis=0, tiled=True)
    out_grad, _ = lax.optimization_barrier((out_grad, hidden))
    out_cols = lax.all_to_all(out_grad, "dp", 1, 0, tiled=True)
    hid_grad = lax.dot_general(
        out_grad, w_out, (((1,), (1,)), ((), ())), preferred_element_type=jnp.float32
    )
    pre_grad = (hid_grad * slope).astype(jnp.bfloat16)
    pre_grad_all = lax.all_gather(pre_grad, "dp", axis=0, tiled=True)
    input_part = lax.dot_general(
        pre_grad, w_in, (((1,), (1,)), ((), ())), preferred_element_type=jnp.float32
    )
    inputs, input_part = lax.optimization_barrier((inputs, input_part))
    in_cols = lax.all_to_all(inputs, "dp", 1, 0, tiled=True)
    pieces = scatter_pieces(input_part, "mp")

    grad_out = contract_rows(hidden_all, out_cols)
    square_out = grad_out * grad_out + tiny_square
    width_out, row_out_sum = lax.psum((jnp.sum(square_out, axis=0), jnp.sum(row_out)), "mp")
    cols_out = decay_rate * col_out + (1.0 - decay_rate) * width_out / FF
    hidden_out, sum_out = lax.psum((jnp.sum(square_out, axis=1), jnp.sum(width_out)), "dp")
    rows_out = decay_rate * row_out + (1.0 - decay_rate) * hidden_out / D
    mean_out = (decay_rate * row_out_sum + (1.0 - decay_rate) * sum_out / D) / FF
    update_out = grad_out / jnp.sqrt(rows_out[:, None] * cols_out[None, :] / mean_out)
    new_master_out = master_out - step_size * update_out

    pre_grad_all, new_master_out, pieces = lax.optimization_barrier(
        (pre_grad_all, new_master_out, pieces)
    )
    input_grad = sum(piece.astype(jnp.float32) for piece in pieces).astype(jnp.bfloat16)
    grad_in = with_layout_constraint(contract_rows(in_cols, pre_grad_all), Layout((0, 1)))
    square_in = grad_in * grad_in + tiny_square
    width_in = lax.psum(jnp.sum(square_in, axis=1), "mp")
    rows_in = decay_rate * row_in + (1.0 - decay_rate) * width_in / FF
    hidden_in, sum_in = lax.psum((jnp.sum(square_in, axis=0), jnp.sum(rows_in)), "dp")
    cols_in = decay_rate * col_in + (1.0 - decay_rate) * hidden_in / D
    mean_in = sum_in / D
    update_in = grad_in / jnp.sqrt(rows_in[:, None] * cols_in[None, :] / mean_in)
    new_master_in = master_in - step_size * update_in
    return (input_grad, new_master_in, new_master_out)


MESH = pl.DeviceIdType.MESH
NT = (((1,), (1,)), ((), ()))
NN = (((1,), (0,)), ((), ()))
LANES = 128


def dot(left, right, dims):
    return lax.dot_general(left, right, dims, preferred_element_type=jnp.float32)


class Copies:
    def __init__(self, sems, away):
        self.sems = sems
        self.away = away
        self.count = 0
        self.sent = []

    def take(self, number=None):
        first = self.count
        self.count += number or 1
        assert self.count <= SEMAPHORES
        return first if number is None else range(first, self.count)

    def local(self, src, dst, sem):
        pltpu.make_async_copy(src, dst, self.sems.at[sem]).start()

    def settled(self, region, sem):
        pltpu.make_async_copy(region, region, self.sems.at[sem]).wait()

    def sends(self, *regions):
        sem = self.take()
        self.sent += [(region, sem) for region in regions]
        return sem

    def moved(self, src, dst, send, recv, device):
        return pltpu.make_async_remote_copy(
            src_ref=src,
            dst_ref=dst,
            send_sem=self.sems.at[send],
            recv_sem=self.sems.at[recv],
            device_id=device,
            device_id_type=MESH,
        )

    def remote(self, src, dst, send, recv, **device):
        self.moved(src, dst, send, recv, device).start()

    def arrived(self, region, recv):
        self.moved(region, region, recv, recv, self.away).wait_recv()

    def drain(self):
        for region, sem in self.sent:
            self.moved(region, region, sem, sem, self.away).wait_send()


def step_kernel(
    plan,
    og_hbm, pa_hbm, in_hbm, wo_hbm, wi_hbm, ro_hbm, co_hbm, ri_hbm, ci_hbm,
    go, gi, fac, igb,
    og2, pa2, hid, pre, oc, ic, ict, wb, rpb, racc, vec_d, vec_m,
    row_out, col_out, row_in, col_in, sems,
):
    n_dp, n_mp, tok, width, ff, cols, parts = plan
    half, depth = ff // 2, width // 2
    piece = width // n_mp
    chunk = half // parts
    d, z = lax.axis_index("dp"), lax.axis_index("mp")
    core, chip = lax.rem(d, 2), d // 2
    base = pl.multiple_of(chip * 2 * tok, 2 * tok)
    flip = lambda index: d + sum(
        bit * (1 - 2 * lax.rem(d // bit, 2)) for bit in (1, 2, 4) if index & bit
    )
    turn = lambda index: z + sum(
        bit * (1 - 2 * lax.rem(z // bit, 2)) for bit in (1, 2) if index & bit
    )
    dp_of = {index: flip(index) for index in range(1, n_dp)}
    mp_of = {index: turn(index) for index in range(1, n_mp)}
    on = lambda index: dict(dp=dp_of[index], mp=z)

    barrier = pltpu.get_barrier_semaphore()
    for index in range(1, n_dp):
        pl.semaphore_signal(barrier, inc=1, device_id=on(index), device_id_type=MESH)
    for index in range(1, n_mp):
        for peer in (d, dp_of[1]):
            device = dict(dp=peer, mp=mp_of[index])
            pl.semaphore_signal(barrier, inc=1, device_id=device, device_id_type=MESH)

    c = Copies(sems, on(1))
    rows_of = lambda who: pl.ds(pl.multiple_of(who * tok, tok), tok)
    mine = pl.ds(pl.multiple_of(core * tok, tok), tok)
    other = pl.ds(pl.multiple_of((1 - core) * tok, tok), tok)
    half_cols = lambda which: pl.ds(pl.multiple_of(which * half, half), half)
    l_pa, l_og, l_oc, l_ic = (c.take() for _ in range(4))
    own_cols = pl.ds(pl.multiple_of(d * cols, cols), cols)
    c.local(pa_hbm.at[:, half_cols(core)], pa2.at[mine], l_pa)
    c.local(og_hbm, og2.at[mine], l_og)

    side = width // ff
    slots = wb.shape[0]
    in_rows = side * chunk
    n_out, n_in = half // chunk, depth // in_rows
    w_sems = c.take(slots)[0]

    def fetch(item):
        slot = item % slots
        if item < n_out:
            rows = pl.ds(pl.multiple_of(core * half + item * chunk, chunk), chunk)
            c.local(wo_hbm.at[rows], wb.at[slot], w_sems + slot)
        elif item < n_out + n_in:
            for part in range(side):
                at = core * depth + (item - n_out) * in_rows + part * chunk
                rows = pl.ds(pl.multiple_of(at, chunk), chunk)
                to = wb.at[slot, :, pl.ds(part * ff, ff)]
                c.local(wi_hbm.at[rows], to, w_sems + slot)

    fetched = lambda item: c.settled(wb.at[item % slots], w_sems + item % slots)
    for item in range(slots):
        fetch(item)
    c.local(og_hbm.at[:, own_cols], oc.at[rows_of(d)], l_oc)
    c.local(in_hbm.at[:, own_cols], ic.at[rows_of(d)], l_ic)
    vectors = ((ro_hbm, row_out), (co_hbm, col_out), (ri_hbm, row_in), (ci_hbm, col_in))
    l_vectors = c.take(4)
    for (src, dst), sem in zip(vectors, l_vectors):
        c.local(src, dst, sem)

    pl.semaphore_wait(barrier, n_dp - 1 + 2 * (n_mp - 1))

    even = lax.rem(z, 2)
    part_rows = lambda who, which: pl.ds(
        pl.multiple_of(who * tok + which * (tok // 2), tok // 2), tok // 2
    )
    beside = dict(dp=d, mp=mp_of[1])

    def spread(src, dst):
        near, beyond, partner = c.take(3)
        send = c.sends(dst.at[pl.ds(0, (n_dp - 1) * tok)])
        for index in (2, 4, 6, 3, 5, 7):
            their = pl.ds(pl.multiple_of(dp_of[index] * cols, cols), cols)
            c.remote(src.at[part_rows(0, even), their], dst.at[part_rows(d, even)], send, near, **on(index))
        their = pl.ds(pl.multiple_of(dp_of[1] * cols, cols), cols)
        c.remote(src.at[:, their], dst.at[rows_of(d)], send, partner, **on(1))

        def hand_on():
            c.arrived(dst.at[pl.ds(0, (n_dp - 2) * (tok // 2))], near)
            for index in range(2, n_dp):
                rows = dst.at[part_rows(dp_of[index], even)]
                c.remote(rows, rows, send, beyond, **beside)

        def gathered():
            c.arrived(dst.at[rows_of(dp_of[1])], partner)
            c.arrived(dst.at[pl.ds(0, (n_dp - 2) * (tok // 2))], beyond)

        return hand_on, gathered

    hand_on_oc, gathered_oc = spread(og_hbm, oc)
    r_pa, r_og = c.take(2)
    c.remote(
        pa_hbm.at[:, half_cols(1 - core)], pa2.at[mine], c.sends(pa2.at[mine]), r_pa, **on(1)
    )
    c.remote(og_hbm, og2.at[mine], c.sends(og2.at[mine]), r_og, **on(1))
    hand_on_ic, gathered_ic = spread(in_hbm, ic)

    def block(dst, index, which, k):
        tokens = pl.ds(pl.multiple_of((dp_of[index] if index else d) // 2 * 2 * tok, 2 * tok), 2 * tok)
        units = pl.ds(pl.multiple_of(which * half + k * chunk, chunk), chunk)
        return dst.at[units, tokens] if dst is hid else dst.at[tokens, units]

    class Stream:
        def __init__(self, dst):
            self.dst = dst
            self.near = {index: c.take(parts) for index in (2, 4, 6)}
            self.pairs = {index: c.take() for index in (0, 2, 4)}
            self.pairs[6] = c.take(parts)
            units, tokens = pl.ds(0, parts // 2 * 3 * chunk), pl.ds(0, 2 * tok)
            some = dst.at[units, tokens] if dst is hid else dst.at[tokens, units]
            whole = pl.ds(0, n_dp // 2 * tok)
            most = dst.at[:, whole] if dst is hid else dst.at[whole, :]
            self.send = {2: c.sends(some), 4: c.sends(some), 1: c.sends(most)}

        def across(self, index, k):
            return self.pairs[6][k] if index == 6 else self.pairs[index]

        def own(self, k, index):
            src = block(self.dst, 0, core, k)
            recv = self.pairs[0] if index == 1 else self.near[index][k]
            c.remote(src, src, self.send[index], recv, **on(index))

        def pass_on(self, index, k):
            src = block(self.dst, index, core, k)
            c.arrived(src, self.near[index][k])
            if index == 2 and k < parts // 2:
                c.remote(src, src, self.send[4], self.near[6][k], **on(4))
            if index == 4 and k >= parts // 2:
                c.remote(src, src, self.send[2], self.near[6][k], **on(2))
            c.remote(src, src, self.send[1], self.across(index, k), **on(1))

        def whole_from_partner(self, index):
            tokens = pl.ds(pl.multiple_of((dp_of[index] if index else d) // 2 * 2 * tok, 2 * tok), 2 * tok)
            units = half_cols(1 - core)
            region = self.dst.at[units, tokens] if self.dst is hid else self.dst.at[tokens, units]
            c.arrived(region, self.pairs[index])

        def diagonal_from_partner(self, k):
            c.arrived(block(self.dst, 6, 1 - core, k), self.pairs[6][k])

    h_flow, p_flow = Stream(hid), Stream(pre)
    c.settled(pa2.at[mine], l_pa)
    c.arrived(pa2.at[other], r_pa)

    for k in range(parts):
        units = slice(k * chunk, (k + 1) * chunk)
        active, _ = gelu_parts(pa2[:, units].astype(jnp.float32))
        target = pl.ds(pl.multiple_of(core * half + k * chunk, chunk), chunk)
        hid[target, pl.ds(base, 2 * tok)] = active.T.astype(jnp.bfloat16)
        if k:
            for index in (2, 4, 1):
                h_flow.own(k - 1, index)
    c.settled(og2.at[mine], l_og)
    c.arrived(og2.at[other], r_og)
    for k in range(parts):
        fetched(k)
        hid_grad = dot(og2[...], wb[k % slots], NT)
        _, slope = gelu_parts(pa2[:, k * chunk : (k + 1) * chunk].astype(jnp.float32))
        target = pl.ds(pl.multiple_of(core * half + k * chunk, chunk), chunk)
        pre[pl.ds(base, 2 * tok), target] = (hid_grad * slope).astype(jnp.bfloat16)
        fetch(k + slots)
        if k:
            p_flow.own(k - 1, 1)
        else:
            for index in (2, 4, 1):
                h_flow.own(parts - 1, index)
    hand_on_oc()
    p_flow.own(parts - 1, 1)
    p_flow.whole_from_partner(0)

    r_rp = c.take(n_mp)[0]
    owned = n_mp // 2
    s_rp = c.take(owned * 2)[0]

    def piece_copy(which, t):
        to = core * owned + which
        return pltpu.make_async_remote_copy(
            src_ref=og2.at[pl.ds(t * tok, tok), pl.ds(which * piece, piece)],
            dst_ref=rpb.at[z],
            send_sem=sems.at[s_rp + which * 2 + t],
            recv_sem=sems.at[r_rp + z],
            device_id=dict(dp=chip * 2 + t, mp=to),
            device_id_type=MESH,
        ), jnp.logical_or(to != z, core != t)

    def send_pieces(which):
        for t in range(2):
            copy, away = piece_copy(which, t)

            @pl.when(away)
            def _():
                copy.start()

    for k in range(n_in):
        item = n_out + k
        fetched(item)
        for part in range(side):
            rows = wb[item % slots, :, part * ff : (part + 1) * ff]
            value = dot(pre[pl.ds(base, 2 * tok), :], rows, NT).astype(jnp.bfloat16)
            at = k * in_rows + part * chunk
            og2[:, at : at + chunk] = value
        fetch(item + slots)
    hand_on_ic()

    for k in range(parts):
        h_flow.pass_on(2, k)
        h_flow.pass_on(4, k)
        if k == parts // 2 - 1:
            for j in range(parts):
                p_flow.own(j, 4)
        if k >= parts - owned:
            send_pieces(k - parts + owned)
    for k in range(parts):
        p_flow.own(k, 2)
    for (_, dst), sem in zip(vectors, l_vectors):
        c.settled(dst, sem)
    c.settled(oc.at[rows_of(d)], l_oc)
    c.settled(ic.at[rows_of(d)], l_ic)
    for k in range(parts // 2):
        h_flow.pass_on(6, k)
        h_flow.pass_on(6, k + parts // 2)
    gathered_oc()
    for index in (0, 2, 4):
        h_flow.whole_from_partner(index)
    for k in range(parts):
        h_flow.diagonal_from_partner(k)

    def as_rows(row, ref, at):
        for j in range(row.shape[1] // LANES):
            ref[pl.ds(at + j, 1), :] = row[:, j * LANES : (j + 1) * LANES]

    out_rows = 2 * chunk
    fac[...] = jnp.zeros_like(fac)
    zero_m = jnp.zeros((vec_m.shape[1], LANES), jnp.float32)
    for slot in (0, 1):
        vec_m[slot * n_mp] = zero_m
    width_sum = jnp.zeros((1, cols), jnp.float32)
    for k in range(parts):
        rows = slice(k * out_rows, (k + 1) * out_rows)
        grad = dot(hid[rows, :], oc[...], NN)
        square = grad * grad + tiny_square
        width_sum += jnp.sum(square, axis=0, keepdims=True)
        lanes = sum(square[:, j * LANES : (j + 1) * LANES] for j in range(cols // LANES))
        as_rows(jnp.sum(lanes.T, axis=0, keepdims=True), vec_d.at[0], k * out_rows // LANES)
        go[rows, :] = grad.astype(jnp.bfloat16)
        p_flow.pass_on(2, k)
        p_flow.pass_on(4, k)
    gathered_ic()
    ict[...] = ic[...].astype(jnp.float32).T.astype(jnp.bfloat16)
    as_rows(width_sum, vec_m.at[0], 0)

    def exchange(table, slot, peers, height):
        recv = c.take()
        first = slot * (len(peers) + 1)
        rows = pl.ds(0, height)
        there = table.at[pl.ds(first + 1, len(peers)), rows]
        send = c.sends(there)
        for at, device in enumerate(peers):
            c.remote(table.at[first, rows], table.at[first + 1 + at, rows], send, recv, **device)

        def total():
            c.arrived(there, recv)
            return sum(table[first + at, :height] for at in range(len(peers) + 1))

        return total

    dp_peers = [on(index) for index in range(1, n_dp)]
    mp_peers = [dict(dp=d, mp=mp_of[index]) for index in range(1, n_mp)]
    exchange_d = lambda slot, height: exchange(vec_d, slot, dp_peers, height)
    exchange_m = lambda slot: exchange(vec_m, slot, mp_peers, vec_m.shape[1])
    high = ff // LANES
    hidden_out = exchange_d(0, high)
    width_out = exchange_m(0)

    racc[...] = jnp.zeros_like(racc)

    def grad_in(which, k):
        units = pl.ds(pl.multiple_of(which * half + k * chunk, chunk), chunk)
        at = which * parts + k
        grad = dot(ict[...], pre[:, units], NN)
        square = grad * grad + tiny_square
        as_rows(jnp.sum(square, axis=0, keepdims=True), vec_d.at[n_dp], at * chunk // LANES)
        racc[...] += sum(square[:, j * LANES : (j + 1) * LANES] for j in range(chunk // LANES))
        gi[:, units] = grad.astype(jnp.bfloat16)

    for index in (2, 4):
        p_flow.whole_from_partner(index)
    for k in range(parts // 2):
        ready = (k, k + parts // 2)
        for j in ready:
            p_flow.pass_on(6, j)
        for j in ready:
            grad_in(core, j)
        for j in ready:
            p_flow.diagonal_from_partner(j)
        for j in ready:
            grad_in(1 - core, j)
    as_rows(jnp.sum(racc[...].T, axis=0, keepdims=True), vec_m.at[n_mp], 0)
    width_in = exchange_m(1)
    hidden_in = exchange_d(1, high)
    low = cols // LANES
    rows_out = decay_rate * row_out[...] + (1.0 - decay_rate) * hidden_out() / width
    vec_m[2 * n_mp] = jnp.broadcast_to(jnp.sum(rows_out), vec_m.shape[1:])
    cols_out = decay_rate * col_out[...] + (1.0 - decay_rate) * width_out()[:low] / (ff * n_mp)
    for s in range(n_mp):
        gone = jnp.logical_or(s != z, core != z // owned)

        @pl.when(gone)
        def _():
            c.arrived(rpb.at[s], r_rp + s)

    sum_rows = exchange_m(2)

    @pl.when(core == z // owned)
    def _():
        there = pl.ds(pl.multiple_of((z - core * owned) * piece, piece), piece)
        rpb[z] = og2[mine, there]

    rows_in = decay_rate * row_in[...] + (1.0 - decay_rate) * width_in()[:low] / (ff * n_mp)
    vec_d[2 * n_dp, :8] = jnp.broadcast_to(jnp.sum(rows_in), (8, LANES))
    igb[...] = sum(rpb[s].astype(jnp.float32) for s in range(n_mp)).astype(jnp.bfloat16)
    sum_rows_in = exchange_d(2, 8)
    fac[high : 2 * high] = lax.rsqrt(
        decay_rate * col_in[...] + (1.0 - decay_rate) * hidden_in() / width
    )
    fac[2 * high : 2 * high + low] = lax.rsqrt(cols_out)
    mean_out = sum_rows() / (ff * n_mp)
    fac[:high] = step_size * lax.rsqrt(rows_out / mean_out[0:1, :])
    mean_in = sum_rows_in() / width
    fac[2 * high + 8 : 2 * high + 8 + low] = step_size * lax.rsqrt(rows_in / mean_in[0:1, :])
    for which in range(owned):
        for t in range(2):
            copy, away = piece_copy(which, t)

            @pl.when(away)
            def _():
                copy.wait_send()

    c.drain()


def update_kernel(plan, mo, mi, go, gi, fac, ig, new_ig, new_out, new_in, out_b, in_b, sems):
    ff, cols, tiles = plan
    high, low = ff // LANES, cols // LANES
    stores = [pltpu.make_async_copy(ig, new_ig, sems.at[2 * tiles])]
    stores[0].start()
    turned = fac[...].T
    for new, old, stage, grad, first, height, across, rows_at, cols_at in (
        (new_out, mo, out_b, go, 0, high, low, 0, 2 * high),
        (new_in, mi, in_b, gi, tiles, low, high, 2 * high + 8, high),
    ):
        for tile in range(tiles):
            bands = range(tile * height // tiles, (tile + 1) * height // tiles)
            for band in bands:
                rows = slice(band * LANES, (band + 1) * LANES)
                down = jnp.broadcast_to(turned[:, rows_at + band : rows_at + band + 1], (LANES, LANES))

                def lane_group(j, carry):
                    at = pl.ds(pl.multiple_of(j * LANES, LANES), LANES)
                    scale = down * fac[pl.ds(cols_at + j, 1), :]
                    stage[rows, at] = old[rows, at] - grad[rows, at].astype(jnp.float32) * scale
                    return carry

                lax.fori_loop(0, across, lane_group, 0, unroll=3)
            rows = slice(bands[0] * LANES, (bands[-1] + 1) * LANES)
            stores.append(pltpu.make_async_copy(stage.at[rows], new.at[rows], sems.at[first + tile]))
            stores[-1].start()
    for store in stores:
        store.wait()


def fast_body(n_dp, n_mp, inputs, pre_act, out_grad, w_in, w_out, master_in, master_out, row_in, col_in, row_out, col_out):
    tok, width = inputs.shape
    ff = pre_act.shape[1]
    cols = width // n_dp
    parts = PARTS
    chunk = ff // 2 // parts
    high, low = ff // LANES, cols // LANES
    slots, tiles = 2, math.gcd(high, low)
    bf, f32 = jnp.bfloat16, jnp.float32
    anywhere = pl.BlockSpec(memory_space=pl.ANY)
    vmem = pl.BlockSpec(memory_space=pltpu.VMEM)
    shape = jax.ShapeDtypeStruct
    plan = (n_dp, n_mp, tok, width, ff, cols, parts)
    in_hbm = lambda array: pltpu.with_memory_space_constraint(array, pltpu.HBM)
    in_vmem = lambda array: pltpu.with_memory_space_constraint(array, pltpu.VMEM)
    held = pl.pallas_call(
        functools.partial(step_kernel, plan),
        out_shape=(
            pltpu.VMEM((ff, cols), bf),
            pltpu.VMEM((cols, ff), bf),
            pltpu.VMEM((2 * high + 16, LANES), f32),
            pltpu.VMEM((tok, width // n_mp), bf),
        ),
        in_specs=[anywhere] * 9,
        out_specs=(vmem,) * 4,
        scratch_shapes=[
            pltpu.VMEM((2 * tok, width), bf),
            pltpu.VMEM((2 * tok, ff // 2), bf),
            pltpu.VMEM((ff, n_dp * tok), bf),
            pltpu.VMEM((n_dp * tok, ff), bf),
            pltpu.VMEM((n_dp * tok, cols), bf),
            pltpu.VMEM((n_dp * tok, cols), bf),
            pltpu.VMEM((cols, n_dp * tok), bf),
            pltpu.VMEM((slots, chunk, width), bf),
            pltpu.VMEM((n_mp, tok, width // n_mp), bf),
            pltpu.VMEM((cols, LANES), f32),
            pltpu.VMEM((3 * n_dp, high, LANES), f32),
            pltpu.VMEM((3 * n_mp, 8, LANES), f32),
            pltpu.VMEM((high, LANES), f32),
            pltpu.VMEM((low, LANES), f32),
            pltpu.VMEM((low, LANES), f32),
            pltpu.VMEM((high, LANES), f32),
            pltpu.SemaphoreType.DMA((SEMAPHORES,)),
        ],
        compiler_params=pltpu.CompilerParams(
            collective_id=0, has_side_effects=True, vmem_limit_bytes=K1_VMEM
        ),
    )(
        *map(
            in_hbm,
            (
                out_grad, pre_act, inputs, w_out, w_in,
                row_out.reshape(high, LANES), col_out.reshape(low, LANES),
                row_in.reshape(low, LANES), col_in.reshape(high, LANES),
            ),
        )
    )
    new_ig, new_master_out, new_master_in = pl.pallas_call(
        functools.partial(update_kernel, (ff, cols, tiles)),
        out_shape=(shape((tok, width // n_mp), bf), shape((ff, cols), f32), shape((cols, ff), f32)),
        in_specs=[vmem] * 6,
        out_specs=(anywhere,) * 3,
        scratch_shapes=[
            pltpu.VMEM((ff, cols), f32),
            pltpu.VMEM((cols, ff), f32),
            pltpu.SemaphoreType.DMA((2 * tiles + 1,)),
        ],
        compiler_params=pltpu.CompilerParams(vmem_limit_bytes=K2_VMEM),
    )(*map(in_vmem, (master_out, master_in, *held)))
    return new_ig, new_master_in, new_master_out


SEMAPHORES = 102
K1_VMEM = 30 * 2**20
K2_VMEM = 21 * 2**20
PARTS = 6


def fits(mesh):
    n_dp, n_mp = mesh.shape["dp"], mesh.shape["mp"]
    return n_dp == 8 and n_mp == 4 and D % (n_dp * LANES) == 0 and D <= 8 * n_dp * LANES and D * n_mp % FF == 0 and FF % (n_mp * 2 * PARTS * LANES) == 0


def solution(mesh):
    in_specs = (
        P("dp", None),
        P("dp", "mp"),
        P("dp", None),
        P(None, "mp"),
        P("mp", None),
        P("dp", "mp"),
        P("mp", "dp"),
        P("dp"),
        P("mp"),
        P("mp"),
        P("dp"),
    )
    out_specs = (P("dp", "mp"), P("dp", "mp"), P("mp", "dp"))
    run = body
    if fits(mesh):
        run = functools.partial(fast_body, mesh.shape["dp"], mesh.shape["mp"])
    return jax.shard_map(run, mesh=mesh, in_specs=in_specs, out_specs=out_specs, check_vma=False)
```

```python
import functools
import math

import jax
import jax.numpy as jnp
from jax import lax
from jax.experimental import pallas as pl
from jax.experimental.pallas import tpu as pltpu
from jax.experimental.layout import Layout, with_layout_constraint
from jax.sharding import PartitionSpec as P

D = 6144
FF = 12288


decay_rate = 0.8
step_size = 0.05
tiny_square = 1e-30


def gelu_parts(pre):
    cumulative = 0.5 * (1.0 + jax.scipy.special.erf(pre * (1.0 / math.sqrt(2.0))))
    density = jnp.exp(-0.5 * pre * pre) * (1.0 / math.sqrt(2.0 * math.pi))
    return (pre * cumulative, cumulative + pre * density)


def contract_rows(left, right):
    return lax.dot_general(
        left, right, (((0,), (0,)), ((), ())), preferred_element_type=jnp.float32
    )


def scatter_pieces(partial, axis):
    size = lax.axis_size(axis)
    me = lax.axis_index(axis)
    width = partial.shape[1] // size
    piece = lambda k: lax.dynamic_slice_in_dim(partial, k * width, width, 1)
    pieces = [piece(me)]
    for shift in range(1, size):
        moved = piece(lax.rem(me + shift, size)).astype(jnp.bfloat16)
        pieces.append(lax.ppermute(moved, axis, [(i, (i + shift) % size) for i in range(size)]))
    return pieces


def body(
    inputs, pre_act, out_grad, w_in, w_out, master_in, master_out, row_in, col_in, row_out, col_out
):
    active, slope = gelu_parts(pre_act.astype(jnp.float32))
    hidden = active.astype(jnp.bfloat16)
    hidden_all = lax.all_gather(hidden, "dp", axis=0, tiled=True)
    out_grad, _ = lax.optimization_barrier((out_grad, hidden))
    out_cols = lax.all_to_all(out_grad, "dp", 1, 0, tiled=True)
    hid_grad = lax.dot_general(
        out_grad, w_out, (((1,), (1,)), ((), ())), preferred_element_type=jnp.float32
    )
    pre_grad = (hid_grad * slope).astype(jnp.bfloat16)
    pre_grad_all = lax.all_gather(pre_grad, "dp", axis=0, tiled=True)
    input_part = lax.dot_general(
        pre_grad, w_in, (((1,), (1,)), ((), ())), preferred_element_type=jnp.float32
    )
    inputs, input_part = lax.optimization_barrier((inputs, input_part))
    in_cols = lax.all_to_all(inputs, "dp", 1, 0, tiled=True)
    pieces = scatter_pieces(input_part, "mp")

    grad_out = contract_rows(hidden_all, out_cols)
    square_out = grad_out * grad_out + tiny_square
    width_out, row_out_sum = lax.psum((jnp.sum(square_out, axis=0), jnp.sum(row_out)), "mp")
    cols_out = decay_rate * col_out + (1.0 - decay_rate) * width_out / FF
    hidden_out, sum_out = lax.psum((jnp.sum(square_out, axis=1), jnp.sum(width_out)), "dp")
    rows_out = decay_rate * row_out + (1.0 - decay_rate) * hidden_out / D
    mean_out = (decay_rate * row_out_sum + (1.0 - decay_rate) * sum_out / D) / FF
    update_out = grad_out / jnp.sqrt(rows_out[:, None] * cols_out[None, :] / mean_out)
    new_master_out = master_out - step_size * update_out

    pre_grad_all, new_master_out, pieces = lax.optimization_barrier(
        (pre_grad_all, new_master_out, pieces)
    )
    input_grad = sum(piece.astype(jnp.float32) for piece in pieces).astype(jnp.bfloat16)
    grad_in = with_layout_constraint(contract_rows(in_cols, pre_grad_all), Layout((0, 1)))
    square_in = grad_in * grad_in + tiny_square
    width_in = lax.psum(jnp.sum(square_in, axis=1), "mp")
    rows_in = decay_rate * row_in + (1.0 - decay_rate) * width_in / FF
    hidden_in, sum_in = lax.psum((jnp.sum(square_in, axis=0), jnp.sum(rows_in)), "dp")
    cols_in = decay_rate * col_in + (1.0 - decay_rate) * hidden_in / D
    mean_in = sum_in / D
    update_in = grad_in / jnp.sqrt(rows_in[:, None] * cols_in[None, :] / mean_in)
    new_master_in = master_in - step_size * update_in
    return (input_grad, new_master_in, new_master_out)


MESH = pl.DeviceIdType.MESH
NT = (((1,), (1,)), ((), ()))
NN = (((1,), (0,)), ((), ()))
LANES = 128


def dot(left, right, dims):
    return lax.dot_general(left, right, dims, preferred_element_type=jnp.float32)


class Copies:
    def __init__(self, sems, away):
        self.sems = sems
        self.away = away
        self.count = 0
        self.sent = []

    def take(self, number=None):
        first = self.count
        self.count += number or 1
        assert self.count <= SEMAPHORES
        return first if number is None else range(first, self.count)

    def local(self, src, dst, sem):
        pltpu.make_async_copy(src, dst, self.sems.at[sem]).start()

    def settled(self, region, sem):
        pltpu.make_async_copy(region, region, self.sems.at[sem]).wait()

    def sends(self, *regions):
        sem = self.take()
        self.sent += [(region, sem) for region in regions]
        return sem

    def moved(self, src, dst, send, recv, device):
        return pltpu.make_async_remote_copy(
            src_ref=src,
            dst_ref=dst,
            send_sem=self.sems.at[send],
            recv_sem=self.sems.at[recv],
            device_id=device,
            device_id_type=MESH,
        )

    def remote(self, src, dst, send, recv, **device):
        self.moved(src, dst, send, recv, device).start()

    def arrived(self, region, recv):
        self.moved(region, region, recv, recv, self.away).wait_recv()

    def drain(self):
        for region, sem in self.sent:
            self.moved(region, region, sem, sem, self.away).wait_send()


def step_kernel(
    plan,
    og_hbm, pa_hbm, in_hbm, wo_hbm, wi_hbm, ro_hbm, co_hbm, ri_hbm, ci_hbm,
    go, gi, fac, igb,
    og2, pa2, hid, pre, oc, ic, ict, wb, rpb, racc, vec_d, vec_m,
    row_out, col_out, row_in, col_in, sems,
):
    n_dp, n_mp, tok, width, ff, cols, parts = plan
    half, depth = ff // 2, width // 2
    piece = width // n_mp
    chunk = half // parts
    d, z = lax.axis_index("dp"), lax.axis_index("mp")
    core, chip = lax.rem(d, 2), d // 2
    base = pl.multiple_of(chip * 2 * tok, 2 * tok)
    flip = lambda index: d + sum(
        bit * (1 - 2 * lax.rem(d // bit, 2)) for bit in (1, 2, 4) if index & bit
    )
    turn = lambda index: z + sum(
        bit * (1 - 2 * lax.rem(z // bit, 2)) for bit in (1, 2) if index & bit
    )
    dp_of = {index: flip(index) for index in range(1, n_dp)}
    mp_of = {index: turn(index) for index in range(1, n_mp)}
    on = lambda index: dict(dp=dp_of[index], mp=z)

    barrier = pltpu.get_barrier_semaphore()
    for index in range(1, n_dp):
        pl.semaphore_signal(barrier, inc=1, device_id=on(index), device_id_type=MESH)
    for index in range(1, n_mp):
        for peer in (d, dp_of[1]):
            device = dict(dp=peer, mp=mp_of[index])
            pl.semaphore_signal(barrier, inc=1, device_id=device, device_id_type=MESH)

    c = Copies(sems, on(1))
    rows_of = lambda who: pl.ds(pl.multiple_of(who * tok, tok), tok)
    mine = pl.ds(pl.multiple_of(core * tok, tok), tok)
    other = pl.ds(pl.multiple_of((1 - core) * tok, tok), tok)
    half_cols = lambda which: pl.ds(pl.multiple_of(which * half, half), half)
    l_pa, l_og, l_oc, l_ic = (c.take() for _ in range(4))
    own_cols = pl.ds(pl.multiple_of(d * cols, cols), cols)
    c.local(pa_hbm.at[:, half_cols(core)], pa2.at[mine], l_pa)
    c.local(og_hbm, og2.at[mine], l_og)

    side = width // ff
    slots = wb.shape[0]
    in_rows = side * chunk
    n_out, n_in = half // chunk, depth // in_rows
    w_sems = c.take(slots)[0]

    def fetch(item):
        slot = item % slots
        if item < n_out:
            rows = pl.ds(pl.multiple_of(core * half + item * chunk, chunk), chunk)
            c.local(wo_hbm.at[rows], wb.at[slot], w_sems + slot)
        elif item < n_out + n_in:
            for part in range(side):
                at = core * depth + (item - n_out) * in_rows + part * chunk
                rows = pl.ds(pl.multiple_of(at, chunk), chunk)
                to = wb.at[slot, :, pl.ds(part * ff, ff)]
                c.local(wi_hbm.at[rows], to, w_sems + slot)

    fetched = lambda item: c.settled(wb.at[item % slots], w_sems + item % slots)
    for item in range(slots):
        fetch(item)
    c.local(og_hbm.at[:, own_cols], oc.at[rows_of(d)], l_oc)
    c.local(in_hbm.at[:, own_cols], ic.at[rows_of(d)], l_ic)
    vectors = ((ro_hbm, row_out), (co_hbm, col_out), (ri_hbm, row_in), (ci_hbm, col_in))
    l_vectors = c.take(4)
    for (src, dst), sem in zip(vectors, l_vectors):
        c.local(src, dst, sem)

    pl.semaphore_wait(barrier, n_dp - 1 + 2 * (n_mp - 1))

    even = lax.rem(z, 2)
    part_rows = lambda who, which: pl.ds(
        pl.multiple_of(who * tok + which * (tok // 2), tok // 2), tok // 2
    )
    beside = dict(dp=d, mp=mp_of[1])

    def spread(src, dst):
        near, beyond, partner = c.take(3)
        send = c.sends(dst.at[pl.ds(0, (n_dp - 1) * tok)])
        for index in (2, 4, 6, 3, 5, 7):
            their = pl.ds(pl.multiple_of(dp_of[index] * cols, cols), cols)
            c.remote(src.at[part_rows(0, even), their], dst.at[part_rows(d, even)], send, near, **on(index))
        their = pl.ds(pl.multiple_of(dp_of[1] * cols, cols), cols)
        c.remote(src.at[:, their], dst.at[rows_of(d)], send, partner, **on(1))

        def hand_on():
            c.arrived(dst.at[pl.ds(0, (n_dp - 2) * (tok // 2))], near)
            for index in range(2, n_dp):
                rows = dst.at[part_rows(dp_of[index], even)]
                c.remote(rows, rows, send, beyond, **beside)

        def gathered():
            c.arrived(dst.at[rows_of(dp_of[1])], partner)
            c.arrived(dst.at[pl.ds(0, (n_dp - 2) * (tok // 2))], beyond)

        return hand_on, gathered

    hand_on_oc, gathered_oc = spread(og_hbm, oc)
    r_pa, r_og = c.take(2)
    c.remote(
        pa_hbm.at[:, half_cols(1 - core)], pa2.at[mine], c.sends(pa2.at[mine]), r_pa, **on(1)
    )
    c.remote(og_hbm, og2.at[mine], c.sends(og2.at[mine]), r_og, **on(1))
    hand_on_ic, gathered_ic = spread(in_hbm, ic)

    def block(dst, index, which, k):
        tokens = pl.ds(pl.multiple_of((dp_of[index] if index else d) // 2 * 2 * tok, 2 * tok), 2 * tok)
        units = pl.ds(pl.multiple_of(which * half + k * chunk, chunk), chunk)
        return dst.at[units, tokens] if dst is hid else dst.at[tokens, units]

    class Stream:
        def __init__(self, dst):
            self.dst = dst
            self.near = {index: c.take(parts) for index in (2, 4, 6)}
            self.pairs = {index: c.take() for index in (0, 2, 4)}
            self.pairs[6] = c.take(parts)
            units, tokens = pl.ds(0, parts // 2 * 3 * chunk), pl.ds(0, 2 * tok)
            some = dst.at[units, tokens] if dst is hid else dst.at[tokens, units]
            whole = pl.ds(0, n_dp // 2 * tok)
            most = dst.at[:, whole] if dst is hid else dst.at[whole, :]
            self.send = {2: c.sends(some), 4: c.sends(some), 1: c.sends(most)}

        def across(self, index, k):
            return self.pairs[6][k] if index == 6 else self.pairs[index]

        def own(self, k, index):
            src = block(self.dst, 0, core, k)
            recv = self.pairs[0] if index == 1 else self.near[index][k]
            c.remote(src, src, self.send[index], recv, **on(index))

        def pass_on(self, index, k):
            src = block(self.dst, index, core, k)
            c.arrived(src, self.near[index][k])
            if index == 2 and k < parts // 2:
                c.remote(src, src, self.send[4], self.near[6][k], **on(4))
            if index == 4 and k >= parts // 2:
                c.remote(src, src, self.send[2], self.near[6][k], **on(2))
            c.remote(src, src, self.send[1], self.across(index, k), **on(1))

        def whole_from_partner(self, index):
            tokens = pl.ds(pl.multiple_of((dp_of[index] if index else d) // 2 * 2 * tok, 2 * tok), 2 * tok)
            units = half_cols(1 - core)
            region = self.dst.at[units, tokens] if self.dst is hid else self.dst.at[tokens, units]
            c.arrived(region, self.pairs[index])

        def diagonal_from_partner(self, k):
            c.arrived(block(self.dst, 6, 1 - core, k), self.pairs[6][k])

    h_flow, p_flow = Stream(hid), Stream(pre)
    c.settled(pa2.at[mine], l_pa)
    c.arrived(pa2.at[other], r_pa)

    for k in range(parts):
        units = slice(k * chunk, (k + 1) * chunk)
        active, _ = gelu_parts(pa2[:, units].astype(jnp.float32))
        target = pl.ds(pl.multiple_of(core * half + k * chunk, chunk), chunk)
        hid[target, pl.ds(base, 2 * tok)] = active.T.astype(jnp.bfloat16)
        if k:
            for index in (2, 4, 1):
                h_flow.own(k - 1, index)
    c.settled(og2.at[mine], l_og)
    c.arrived(og2.at[other], r_og)
    for k in range(parts):
        fetched(k)
        hid_grad = dot(og2[...], wb[k % slots], NT)
        _, slope = gelu_parts(pa2[:, k * chunk : (k + 1) * chunk].astype(jnp.float32))
        target = pl.ds(pl.multiple_of(core * half + k * chunk, chunk), chunk)
        pre[pl.ds(base, 2 * tok), target] = (hid_grad * slope).astype(jnp.bfloat16)
        fetch(k + slots)
        if k:
            p_flow.own(k - 1, 1)
        else:
            for index in (2, 4, 1):
                h_flow.own(parts - 1, index)
    hand_on_oc()
    p_flow.own(parts - 1, 1)
    p_flow.whole_from_partner(0)

    r_rp = c.take(n_mp)[0]
    owned = n_mp // 2
    s_rp = c.take(owned * 2)[0]

    def piece_copy(which, t):
        to = core * owned + which
        return pltpu.make_async_remote_copy(
            src_ref=og2.at[pl.ds(t * tok, tok), pl.ds(which * piece, piece)],
            dst_ref=rpb.at[z],
            send_sem=sems.at[s_rp + which * 2 + t],
            recv_sem=sems.at[r_rp + z],
            device_id=dict(dp=chip * 2 + t, mp=to),
            device_id_type=MESH,
        ), jnp.logical_or(to != z, core != t)

    def send_pieces(which):
        for t in range(2):
            copy, away = piece_copy(which, t)

            @pl.when(away)
            def _():
                copy.start()

    for k in range(n_in):
        item = n_out + k
        fetched(item)
        for part in range(side):
            rows = wb[item % slots, :, part * ff : (part + 1) * ff]
            value = dot(pre[pl.ds(base, 2 * tok), :], rows, NT).astype(jnp.bfloat16)
            at = k * in_rows + part * chunk
            og2[:, at : at + chunk] = value
        fetch(item + slots)
    hand_on_ic()

    for k in range(parts):
        h_flow.pass_on(2, k)
        h_flow.pass_on(4, k)
        if k == parts // 2 - 1:
            for j in range(parts):
                p_flow.own(j, 4)
        if k >= parts - owned:
            send_pieces(k - parts + owned)
    for k in range(parts):
        p_flow.own(k, 2)
    for (_, dst), sem in zip(vectors, l_vectors):
        c.settled(dst, sem)
    c.settled(oc.at[rows_of(d)], l_oc)
    c.settled(ic.at[rows_of(d)], l_ic)
    for k in range(parts // 2):
        h_flow.pass_on(6, k)
        h_flow.pass_on(6, k + parts // 2)
    gathered_oc()
    for index in (0, 2, 4):
        h_flow.whole_from_partner(index)
    for k in range(parts):
        h_flow.diagonal_from_partner(k)

    def as_rows(row, ref, at):
        for j in range(row.shape[1] // LANES):
            ref[pl.ds(at + j, 1), :] = row[:, j * LANES : (j + 1) * LANES]

    out_rows = 2 * chunk
    fac[...] = jnp.zeros_like(fac)
    zero_m = jnp.zeros((vec_m.shape[1], LANES), jnp.float32)
    for slot in (0, 1):
        vec_m[slot * n_mp] = zero_m
    width_sum = jnp.zeros((1, cols), jnp.float32)
    for k in range(parts):
        rows = slice(k * out_rows, (k + 1) * out_rows)
        grad = dot(hid[rows, :], oc[...], NN)
        square = grad * grad + tiny_square
        width_sum += jnp.sum(square, axis=0, keepdims=True)
        lanes = sum(square[:, j * LANES : (j + 1) * LANES] for j in range(cols // LANES))
        as_rows(jnp.sum(lanes.T, axis=0, keepdims=True), vec_d.at[0], k * out_rows // LANES)
        go[rows, :] = grad.astype(jnp.bfloat16)
        p_flow.pass_on(2, k)
        p_flow.pass_on(4, k)
    gathered_ic()
    ict[...] = ic[...].astype(jnp.float32).T.astype(jnp.bfloat16)
    as_rows(width_sum, vec_m.at[0], 0)

    def exchange(table, slot, peers, height):
        recv = c.take()
        first = slot * (len(peers) + 1)
        rows = pl.ds(0, height)
        there = table.at[pl.ds(first + 1, len(peers)), rows]
        send = c.sends(there)
        for at, device in enumerate(peers):
            c.remote(table.at[first, rows], table.at[first + 1 + at, rows], send, recv, **device)

        def total():
            c.arrived(there, recv)
            return sum(table[first + at, :height] for at in range(len(peers) + 1))

        return total

    dp_peers = [on(index) for index in range(1, n_dp)]
    mp_peers = [dict(dp=d, mp=mp_of[index]) for index in range(1, n_mp)]
    exchange_d = lambda slot, height: exchange(vec_d, slot, dp_peers, height)
    exchange_m = lambda slot: exchange(vec_m, slot, mp_peers, vec_m.shape[1])
    high = ff // LANES
    hidden_out = exchange_d(0, high)
    width_out = exchange_m(0)

    racc[...] = jnp.zeros_like(racc)

    def grad_in(which, k):
        units = pl.ds(pl.multiple_of(which * half + k * chunk, chunk), chunk)
        at = which * parts + k
        grad = dot(ict[...], pre[:, units], NN)
        square = grad * grad + tiny_square
        as_rows(jnp.sum(square, axis=0, keepdims=True), vec_d.at[n_dp], at * chunk // LANES)
        racc[...] += sum(square[:, j * LANES : (j + 1) * LANES] for j in range(chunk // LANES))
        gi[:, units] = grad.astype(jnp.bfloat16)

    for index in (2, 4):
        p_flow.whole_from_partner(index)
    for k in range(parts // 2):
        ready = (k, k + parts // 2)
        for j in ready:
            p_flow.pass_on(6, j)
        for j in ready:
            grad_in(core, j)
        for j in ready:
            p_flow.diagonal_from_partner(j)
        for j in ready:
            grad_in(1 - core, j)
    as_rows(jnp.sum(racc[...].T, axis=0, keepdims=True), vec_m.at[n_mp], 0)
    width_in = exchange_m(1)
    hidden_in = exchange_d(1, high)
    low = cols // LANES
    rows_out = decay_rate * row_out[...] + (1.0 - decay_rate) * hidden_out() / width
    vec_m[2 * n_mp] = jnp.broadcast_to(jnp.sum(rows_out), vec_m.shape[1:])
    cols_out = decay_rate * col_out[...] + (1.0 - decay_rate) * width_out()[:low] / (ff * n_mp)
    for s in range(n_mp):
        gone = jnp.logical_or(s != z, core != z // owned)

        @pl.when(gone)
        def _():
            c.arrived(rpb.at[s], r_rp + s)

    sum_rows = exchange_m(2)

    @pl.when(core == z // owned)
    def _():
        there = pl.ds(pl.multiple_of((z - core * owned) * piece, piece), piece)
        rpb[z] = og2[mine, there]

    rows_in = decay_rate * row_in[...] + (1.0 - decay_rate) * width_in()[:low] / (ff * n_mp)
    vec_d[2 * n_dp, :8] = jnp.broadcast_to(jnp.sum(rows_in), (8, LANES))
    igb[...] = sum(rpb[s].astype(jnp.float32) for s in range(n_mp)).astype(jnp.bfloat16)
    sum_rows_in = exchange_d(2, 8)
    fac[high : 2 * high] = lax.rsqrt(
        decay_rate * col_in[...] + (1.0 - decay_rate) * hidden_in() / width
    )
    fac[2 * high : 2 * high + low] = lax.rsqrt(cols_out)
    mean_out = sum_rows() / (ff * n_mp)
    fac[:high] = step_size * lax.rsqrt(rows_out / mean_out[0:1, :])
    mean_in = sum_rows_in() / width
    fac[2 * high + 8 : 2 * high + 8 + low] = step_size * lax.rsqrt(rows_in / mean_in[0:1, :])
    for which in range(owned):
        for t in range(2):
            copy, away = piece_copy(which, t)

            @pl.when(away)
            def _():
                copy.wait_send()

    c.drain()


def update_kernel(plan, mo, mi, go, gi, fac, ig, new_ig, new_out, new_in, out_b, in_b, downs, sems):
    ff, cols = plan
    high, low = ff // LANES, cols // LANES
    whole = [
        pltpu.make_async_copy(ig, new_ig, sems.at[0]),
        pltpu.make_async_copy(out_b, new_out, sems.at[1]),
        pltpu.make_async_copy(in_b, new_in, sems.at[2]),
    ]
    whole[0].start()
    turned = fac[...].T
    for at, column in enumerate((*range(high), *range(2 * high + 8, 2 * high + 8 + low))):
        downs[at] = jnp.broadcast_to(turned[:, column : column + 1], (LANES, LANES))

    def update(new, old, stage, grad, sem, first, group, groups, cols_at):
        def band(b, carry):
            rows = pl.ds(pl.multiple_of(b * LANES, LANES), LANES)
            down = downs[first + b]

            def lane_groups(g, carry):
                for j in range(group):
                    at = pl.ds(pl.multiple_of((g * group + j) * LANES, LANES), LANES)
                    scale = down * fac[pl.ds(cols_at + g * group + j, 1), :]
                    stage[rows, at] = old[rows, at] - grad[rows, at].astype(jnp.float32) * scale
                return carry

            lax.fori_loop(0, groups, lane_groups, 0)
            pltpu.make_async_copy(stage.at[rows], new.at[rows], sems.at[sem]).start()
            return carry

        lax.fori_loop(0, stage.shape[0] // LANES, band, 0)

    group = math.gcd(high, low)
    update(new_out, mo, out_b, go, 1, 0, group, low // group, 2 * high)
    update(new_in, mi, in_b, gi, 2, high, group, high // group, high)
    for copy in whole:
        copy.wait()


def fast_body(n_dp, n_mp, inputs, pre_act, out_grad, w_in, w_out, master_in, master_out, row_in, col_in, row_out, col_out):
    tok, width = inputs.shape
    ff = pre_act.shape[1]
    cols = width // n_dp
    parts = PARTS
    chunk = ff // 2 // parts
    high, low = ff // LANES, cols // LANES
    slots = 2
    bf, f32 = jnp.bfloat16, jnp.float32
    anywhere = pl.BlockSpec(memory_space=pl.ANY)
    vmem = pl.BlockSpec(memory_space=pltpu.VMEM)
    shape = jax.ShapeDtypeStruct
    plan = (n_dp, n_mp, tok, width, ff, cols, parts)
    in_hbm = lambda array: pltpu.with_memory_space_constraint(array, pltpu.HBM)
    in_vmem = lambda array: pltpu.with_memory_space_constraint(array, pltpu.VMEM)
    held = pl.pallas_call(
        functools.partial(step_kernel, plan),
        out_shape=(
            pltpu.VMEM((ff, cols), bf),
            pltpu.VMEM((cols, ff), bf),
            pltpu.VMEM((2 * high + 16, LANES), f32),
            pltpu.VMEM((tok, width // n_mp), bf),
        ),
        in_specs=[anywhere] * 9,
        out_specs=(vmem,) * 4,
        scratch_shapes=[
            pltpu.VMEM((2 * tok, width), bf),
            pltpu.VMEM((2 * tok, ff // 2), bf),
            pltpu.VMEM((ff, n_dp * tok), bf),
            pltpu.VMEM((n_dp * tok, ff), bf),
            pltpu.VMEM((n_dp * tok, cols), bf),
            pltpu.VMEM((n_dp * tok, cols), bf),
            pltpu.VMEM((cols, n_dp * tok), bf),
            pltpu.VMEM((slots, chunk, width), bf),
            pltpu.VMEM((n_mp, tok, width // n_mp), bf),
            pltpu.VMEM((cols, LANES), f32),
            pltpu.VMEM((3 * n_dp, high, LANES), f32),
            pltpu.VMEM((3 * n_mp, 8, LANES), f32),
            pltpu.VMEM((high, LANES), f32),
            pltpu.VMEM((low, LANES), f32),
            pltpu.VMEM((low, LANES), f32),
            pltpu.VMEM((high, LANES), f32),
            pltpu.SemaphoreType.DMA((SEMAPHORES,)),
        ],
        compiler_params=pltpu.CompilerParams(
            collective_id=0, has_side_effects=True, vmem_limit_bytes=K1_VMEM
        ),
    )(
        *map(
            in_hbm,
            (
                out_grad, pre_act, inputs, w_out, w_in,
                row_out.reshape(high, LANES), col_out.reshape(low, LANES),
                row_in.reshape(low, LANES), col_in.reshape(high, LANES),
            ),
        )
    )
    new_ig, new_master_out, new_master_in = pl.pallas_call(
        functools.partial(update_kernel, (ff, cols)),
        out_shape=(shape((tok, width // n_mp), bf), shape((ff, cols), f32), shape((cols, ff), f32)),
        in_specs=[vmem] * 6,
        out_specs=(anywhere,) * 3,
        scratch_shapes=[
            pltpu.VMEM((ff, cols), f32),
            pltpu.VMEM((cols, ff), f32),
            pltpu.VMEM((high + low, LANES, LANES), f32),
            pltpu.SemaphoreType.DMA((3,)),
        ],
        compiler_params=pltpu.CompilerParams(vmem_limit_bytes=K2_VMEM),
    )(*map(in_vmem, (master_out, master_in, *held)))
    return new_ig, new_master_in, new_master_out


SEMAPHORES = 102
K1_VMEM = 30 * 2**20
K2_VMEM = 21 * 2**20
PARTS = 6


def fits(mesh):
    n_dp, n_mp = mesh.shape["dp"], mesh.shape["mp"]
    return n_dp == 8 and n_mp == 4 and D % (n_dp * LANES) == 0 and D <= 8 * n_dp * LANES and D * n_mp % FF == 0 and FF % (n_mp * 2 * PARTS * LANES) == 0


def solution(mesh):
    in_specs = (
        P("dp", None),
        P("dp", "mp"),
        P("dp", None),
        P(None, "mp"),
        P("mp", None),
        P("dp", "mp"),
        P("mp", "dp"),
        P("dp"),
        P("mp"),
        P("mp"),
        P("dp"),
    )
    out_specs = (P("dp", "mp"), P("dp", "mp"), P("mp", "dp"))
    run = body
    if fits(mesh):
        run = functools.partial(fast_body, mesh.shape["dp"], mesh.shape["mp"])
    return jax.shard_map(run, mesh=mesh, in_specs=in_specs, out_specs=out_specs, check_vma=False)
```
